32 devices in a mesh: cz: 4 (over z), cy: 2 (over y), cx: 4 (over x, core).
Axes of the slice: x: 2, y: 2, z: 4, core: 2. Of those that a mesh axis runs over, the one named last changes fastest.
Arguments:
- x: bfloat16 [1024, 5120], P(('cx', 'cz'), 'cy')
- w1: bfloat16 [5120, 20480], P('cy', ('cz', 'cx'))
- w2: bfloat16 [20480, 5120], P('cz', ('cy', 'cx'))
Outputs:
- output: bfloat16 [1024, 5120], P(('cx', 'cz'), 'cy')
All inputs are finite; a program needn't handle non-finite values.
Results may differ from the reference program's by a relative error of at most 0.0115024.
Values are sent between devices in bfloat16 or wider.
A program may use at most 1 GiB of HBM per device.

```python
import jax
import jax.numpy as jnp

N = 1024
D = 5120
F = 20480


def setup_inputs(seed: int = 0) -> dict:
    k1, k2, k3 = jax.random.split(jax.random.PRNGKey(seed), 3)
    x = jax.random.normal(k1, (N, D), jnp.float32)
    w1 = jax.random.normal(k2, (D, F), jnp.float32) * D ** -0.5
    w2 = jax.random.normal(k3, (F, D), jnp.float32) * F ** -0.5
    return {"x": x.astype(jnp.bfloat16), "w1": w1.astype(jnp.bfloat16), "w2": w2.astype(jnp.bfloat16)}


def reference(x, w1, w2):
    c = jnp.dot(x, w1, preferred_element_type=jnp.float32).astype(jnp.bfloat16)
    h = jax.nn.gelu(c.astype(jnp.float32), approximate=True).astype(jnp.bfloat16)
    return jnp.dot(h, w2, preferred_element_type=jnp.float32).astype(jnp.bfloat16)
```

```python
import functools

import jax
import jax.numpy as jnp
from jax import lax
from jax.experimental import pallas as pl
from jax.experimental.pallas import tpu as pltpu
from jax.sharding import PartitionSpec as P

MESH = pl.DeviceIdType.MESH
LH, LF, LC, L2 = 1, 2, 3, 4
STEPS = 16 + L2 + 1


def kernel(x_ref, w1_ref, w2_ref, o_ref, w1s, w1o, w2, xb, cs, co, cr, hb, zp, zu, zd, ob,
           wsem, xxs, xxr, xus, xds, xzr, xc0s, xc1s, xc2s, xcr, css, crr, hys, hyr, hx0s, hx0r, hx1s, hx1r,
           hc0s, hc0r, hc1s, hc1r, zss, zur, zdr, oss, orr):
    p, y, a = lax.axis_index("cz"), lax.axis_index("cy"), lax.axis_index("cx")
    core, ax = lax.rem(a, 2), a // 2
    rows, half = 16 * 4, w1s.shape[1]
    a_c, a_x, a_d = a + 1 - 2 * core, lax.rem(a + 2, 4), 3 - a
    a_d = lax.rem(a_c + 2, 4)
    ypeer, cpeer, xpeer = {"cy": 1 - y}, {"cx": a_c}, {"cx": a_x}
    up, down = {"cz": lax.rem(p + 1, 4)}, {"cz": lax.rem(p + 3, 4)}
    spot = 2 * core + ax
    mine, theirs = 2 * core, 2 - 2 * core

    def rcopy(src, dst, ss, rs, device):
        return pltpu.make_async_remote_copy(
            src_ref=src, dst_ref=dst, send_sem=ss, recv_sem=rs, device_id=device, device_id_type=MESH)

    def lanes(owner, width):
        return pl.ds(pl.multiple_of(owner * half, 128), width)

    loads = [
        pltpu.make_async_copy(x_ref, xb.at[pl.ds(4 * p, 4), spot], wsem.at[0]),
        pltpu.make_async_copy(w1_ref.at[:, lanes(1 - y, half)], w1s, wsem.at[1]),
        pltpu.make_async_copy(w1_ref.at[:, lanes(y, half)], w1o, wsem.at[2]),
        pltpu.make_async_copy(w2_ref, w2, wsem.at[3]),
    ]
    for load in loads:
        load.start()

    barrier = pltpu.get_barrier_semaphore()
    for device in (ypeer, cpeer, xpeer, {"cx": a_d}):
        pl.semaphore_signal(barrier, inc=1, device_id=device, device_id_type=MESH)

    @pl.when(p < 3)
    def _():
        pl.semaphore_signal(barrier, inc=1, device_id=up, device_id_type=MESH)

    @pl.when(p > 0)
    def _():
        pl.semaphore_signal(barrier, inc=1, device_id=down, device_id_type=MESH)

    @pl.when((p == 0) | (p == 3))
    def _():
        pl.semaphore_wait(barrier, 5)

    @pl.when((p > 0) & (p < 3))
    def _():
        pl.semaphore_wait(barrier, 6)

    def own_to_x(j):
        piece = xb.at[4 * p + j, spot]
        return rcopy(piece, piece, xxs.at[j], xxr.at[j], xpeer)

    def own_to_core(j):
        piece = xb.at[4 * p + j, spot]
        return rcopy(piece, piece, xc0s.at[j], xcr.at[4 * p + j], cpeer)

    def passed_to_core(j):
        piece = xb.at[4 * p + j, 2 * core + 1 - ax]
        return rcopy(piece, piece, xc1s.at[j], xcr.at[4 * p + j], cpeer)

    def x_up(g):
        pair = xb.at[g, pl.ds(mine, 2)]
        return rcopy(pair, pair, xus.at[g], xzr.at[g], up)

    def x_down(g):
        pair = xb.at[g, pl.ds(mine, 2)]
        return rcopy(pair, pair, xds.at[g], xzr.at[g], down)

    def pair_to_core(g):
        pair = xb.at[g, pl.ds(mine, 2)]
        return rcopy(pair, pair, xc2s.at[g], xcr.at[g], cpeer)

    def own_arrived(j):
        piece = xb.at[4 * p + j, 2 * core + 1 - ax]
        rcopy(piece, piece, xxs.at[j], xxr.at[j], xpeer).wait_recv()
        passed_to_core(j).start()

        @pl.when(p < 3)
        def _():
            x_up(4 * p + j).start()

        @pl.when(p > 0)
        def _():
            x_down(4 * p + j).start()

    loads[0].wait()
    for j in range(4):
        own_to_x(j).start()
        own_to_core(j).start()
    own_arrived(0)
    loads[1].wait()
    loads[2].wait()

    def chunk(i):
        q, j = (i + 2) // 4 - 1, lax.rem(i + 2, 4)
        other = jnp.where(p < 2, 1 + q, 2 - q)
        other = jnp.where((p == 1) & (q == 0), 0, other)
        other = jnp.where((p == 2) & (q == 0), 3, other)
        first, last = i < 2, i >= 14
        block = jnp.where(first | last, p, other)
        return 4 * block + jnp.where(first, i, jnp.where(last, i - 12, j))

    def c_send(g):
        return rcopy(cs.at[g], cr.at[g], css, crr.at[g], ypeer)

    def h_piece(g, owner, width):
        return hb.at[g, :, lanes(owner, width)]

    def layer1(g):
        theirs_x = xb.at[g, pl.ds(theirs, 2)]
        rcopy(theirs_x, theirs_x, xc2s.at[g], xcr.at[g], cpeer).wait_recv()
        xv = xb[g].reshape(rows, xb.shape[3])
        cs[g] = jnp.dot(xv, w1s[...], preferred_element_type=jnp.float32)
        c_send(g).start()
        co[g] = jnp.dot(xv, w1o[...], preferred_element_type=jnp.float32)

    def h_to_y(g):
        piece = h_piece(g, 2 * a + y, half)
        return rcopy(piece, piece, hys, hyr.at[g], ypeer)

    def h_to_x(g):
        piece = h_piece(g, 2 * a + y, half)
        return rcopy(piece, piece, hx0s, hx0r.at[g], xpeer)

    def hy_to_x(g):
        piece = h_piece(g, 2 * a + 1 - y, half)
        return rcopy(piece, piece, hx1s, hx1r.at[g], xpeer)

    def h_to_core(g):
        piece = h_piece(g, 2 * a, 2 * half)
        return rcopy(piece, piece, hc0s, hc0r.at[g], cpeer)

    def hx_to_core(g):
        piece = h_piece(g, 2 * a_x, 2 * half)
        return rcopy(piece, piece, hc1s, hc1r.at[g], cpeer)

    def activation(g):
        rcopy(cr.at[g], cr.at[g], css, crr.at[g], ypeer).wait_recv()
        c = (co[g] + cr[g]).astype(jnp.bfloat16).astype(jnp.float32)
        h = jax.nn.gelu(c, approximate=True).astype(jnp.bfloat16)
        hb[g, :, lanes(2 * a + y, half)] = h
        h_to_y(g).start()
        h_to_x(g).start()

    def pass_y(g):
        piece = h_piece(g, 2 * a + 1 - y, half)
        rcopy(piece, piece, hys, hyr.at[g], ypeer).wait_recv()
        hy_to_x(g).start()
        h_to_core(g).start()

    def pass_x(g):
        piece = h_piece(g, 2 * a_x + y, half)
        rcopy(piece, piece, hx0s, hx0r.at[g], xpeer).wait_recv()
        piece = h_piece(g, 2 * a_x + 1 - y, half)
        rcopy(piece, piece, hx1s, hx1r.at[g], xpeer).wait_recv()
        hx_to_core(g).start()

    def layer2(g):
        piece = h_piece(g, 2 * a_c, 2 * half)
        rcopy(piece, piece, hc0s, hc0r.at[g], cpeer).wait_recv()
        piece = h_piece(g, 2 * a_d, 2 * half)
        rcopy(piece, piece, hc1s, hc1r.at[g], cpeer).wait_recv()
        zp[g] = jnp.dot(hb[g], w2[...], preferred_element_type=jnp.float32)

    def z_up(g):
        return rcopy(zp.at[g], zu.at[g], zss.at[g], zur.at[g], up)

    def z_down(g):
        return rcopy(zp.at[g], zd.at[g], zss.at[g], zdr.at[g], down)

    def from_below(g):
        rcopy(zu.at[g], zu.at[g], zss.at[g], zur.at[g], up).wait_recv()

    def from_above(g):
        rcopy(zd.at[g], zd.at[g], zss.at[g], zdr.at[g], down).wait_recv()

    def below_to_up(g):
        from_below(g)
        zp[g] = zp[g] + zu[g]
        z_up(g).start()

    def above_to_down(g):
        from_above(g)
        zp[g] = zp[g] + zd[g]
        z_down(g).start()

    def out_copy(j, e):
        owner = (a_c, a_x, a_d)[e]
        q = 2 * lax.rem(owner, 2) + owner // 2
        return rcopy(ob.at[j, q], o_ref.at[j, :, lanes(a, half)], oss, orr, {"cx": owner})

    def out_own(j):
        return pltpu.make_async_copy(ob.at[j, spot], o_ref.at[j, :, lanes(a, half)], orr)

    def finish(j):
        g = 4 * p + j

        @pl.when(p > 0)
        def _():
            from_below(g)
            zp[g] = zp[g] + zu[g]

        @pl.when(p < 3)
        def _():
            from_above(g)
            zp[g] = zp[g] + zd[g]

        ob[j] = zp[g].astype(jnp.bfloat16).reshape(ob.shape[1:])
        for e in range(3):
            out_copy(j, e).start()
        out_own(j).start()

    edge = (p == 0) | (p == 3)

    def step(s, carry):
        @pl.when(s < 16)
        def _():
            layer1(chunk(s))

        @pl.when((s >= LH) & (s < 16 + LH))
        def _():
            activation(chunk(s - LH))

        @pl.when(s < 3)
        def _():
            own_arrived(s + 1)

        d, jz = (s + 3) // 4, lax.rem(s + 3, 4)

        @pl.when((s >= 1) & (s <= 12) & (p - d >= 0))
        def _():
            g = 4 * (p - d) + jz
            pair = xb.at[g, pl.ds(mine, 2)]
            rcopy(pair, pair, xus.at[g], xzr.at[g], up).wait_recv()

            @pl.when(p < 3)
            def _():
                x_up(g).start()

            pair_to_core(g).start()

        @pl.when((s >= 1) & (s <= 12) & (p + d <= 3))
        def _():
            g = 4 * (p + d) + jz
            pair = xb.at[g, pl.ds(mine, 2)]
            rcopy(pair, pair, xds.at[g], xzr.at[g], down).wait_recv()

            @pl.when(p > 0)
            def _():
                x_down(g).start()

            pair_to_core(g).start()

        t = s - L2

        @pl.when(t == 0)
        def _():
            loads[3].wait()

        @pl.when((t >= 0) & (t < 16))
        def _():
            layer2(chunk(t))

        @pl.when((t >= 2) & (t < 14) & (p == 0))
        def _():
            z_up(chunk(t)).start()

        @pl.when((t >= 2) & (t < 14) & (p == 3))
        def _():
            z_down(chunk(t)).start()

        @pl.when((t >= 7) & (t < 15) & (p == 1))
        def _():
            below_to_up(chunk(t - 1))

        @pl.when((t >= 7) & (t < 15) & (p == 2))
        def _():
            above_to_down(chunk(t - 1))

        @pl.when((t >= 12) & (t < 16) & (p == 1))
        def _():
            above_to_down(chunk(t - 10))

        @pl.when((t >= 12) & (t < 16) & (p == 2))
        def _():
            below_to_up(chunk(t - 10))

        @pl.when((s >= LF) & (s < 16 + LF))
        def _():
            pass_y(chunk(s - LF))

        @pl.when((s >= LC) & (s < 16 + LC))
        def _():
            pass_x(chunk(s - LC))

        @pl.when(t >= 13)
        def _():
            finish(t - 13)

        return carry

    lax.fori_loop(0, STEPS, step, 0)

    rcopy(o_ref, o_ref, oss, orr, cpeer).wait_recv()
    rcopy(ob.at[:, pl.ds(0, 3)], ob.at[:, pl.ds(0, 3)], oss, orr, cpeer).wait_send()
    rcopy(cs, cs, css, crr.at[0], cpeer).wait_send()
    one = hb.at[:, :, pl.ds(0, half)]
    two = hb.at[:, :, pl.ds(0, 2 * half)]
    rcopy(one, one, hys, hyr.at[0], cpeer).wait_send()
    rcopy(one, one, hx0s, hx0r.at[0], cpeer).wait_send()
    rcopy(one, one, hx1s, hx1r.at[0], cpeer).wait_send()
    rcopy(two, two, hc0s, hc0r.at[0], cpeer).wait_send()
    rcopy(two, two, hc1s, hc1r.at[0], cpeer).wait_send()

    def drain(g, carry):
        block = g // 4

        @pl.when(block == p)
        def _():
            j = lax.rem(g, 4)
            own_to_x(j).wait_send()
            own_to_core(j).wait_send()
            passed_to_core(j).wait_send()

        @pl.when(block != p)
        def _():
            pair_to_core(g).wait_send()
            z_up(g).wait_send()

        @pl.when((block <= p) & (p < 3))
        def _():
            x_up(g).wait_send()

        @pl.when((block >= p) & (p > 0))
        def _():
            x_down(g).wait_send()

        return carry

    lax.fori_loop(0, 16, drain, 0)


def solution(mesh):
    def body(x, w1, w2):
        r, d = x.shape
        k1, n1 = w1.shape
        k2, n2 = w2.shape
        half = n1 // 2
        f32, bf16 = jnp.float32, jnp.bfloat16
        dma = pltpu.SemaphoreType.DMA
        out = pl.pallas_call(
            kernel,
            out_shape=jax.ShapeDtypeStruct((4, r // 4, d), bf16),
            in_specs=[pl.BlockSpec(memory_space=pl.ANY)] * 3,
            out_specs=pl.BlockSpec(memory_space=pl.ANY),
            scratch_shapes=[
                pltpu.VMEM((k1, half), bf16),
                pltpu.VMEM((k1, half), bf16),
                pltpu.VMEM((k2, n2), bf16),
                pltpu.VMEM((16, 4, 16, d), bf16),
                pltpu.VMEM((16, 64, half), f32),
                pltpu.VMEM((16, 64, half), f32),
                pltpu.VMEM((16, 64, half), f32),
                pltpu.VMEM((16, 64, k2), bf16),
                pltpu.VMEM((16, 64, n2), f32),
                pltpu.VMEM((16, 64, n2), f32),
                pltpu.VMEM((16, 64, n2), f32),
                pltpu.VMEM((4, 4, 16, n2), bf16),
                dma((4,)),
                dma((4,)), dma((4,)),
                dma((16,)), dma((16,)), dma((16,)),
                dma((4,)), dma((4,)), dma((16,)), dma((16,)),
                dma(()), dma((16,)),
                dma(()), dma((16,)),
                dma(()), dma((16,)),
                dma(()), dma((16,)),
                dma(()), dma((16,)),
                dma(()), dma((16,)),
                dma((16,)), dma((16,)), dma((16,)),
                dma(()), dma(()),
            ],
            compiler_params=pltpu.CompilerParams(
                collective_id=0, has_side_effects=True, vmem_limit_bytes=60 * 1024 * 1024),
            name="mlp",
        )(x.reshape(4, r // 4, d), w1, w2)
        return out.reshape(r, d)

    return jax.shard_map(
        body,
        mesh=mesh,
        in_specs=(P(("cx", "cz"), "cy"), P("cy", ("cz", "cx")), P("cz", ("cy", "cx"))),
        out_specs=P(("cx", "cz"), "cy"),
        check_vma=False,
    )
```

```python
import jax
import jax.numpy as jnp
from jax import lax
from jax.experimental import pallas as pl
from jax.experimental.pallas import tpu as pltpu
from jax.sharding import PartitionSpec as P

MESH = pl.DeviceIdType.MESH
CHUNKS, ROWS = 32, 32
LH, LF, LC, L2 = 2, 4, 5, 7
LZ = 2
EDGE = (0, 2, 4, 5, 6, 7, 3, 1)
MIDDLE = (2, 0, 1, 4, 6, 7, 5, 3)
X_EDGE = ((3, 1, 0), (5, 1, 1), (7, 2, 0), (8, 2, 1), (10, 2, 2), (11, 2, 3), (12, 3, 0), (14, 3, 1), (15, 3, 2), (17, 3, 3),
          (18, 1, 2), (20, 1, 3))
X_BACK = ((3, 0, 0), (5, 0, 1), (6, 0, 2), (8, 0, 3))
X_FRONT = ((3, 2, 0), (5, 2, 1), (6, 2, 2), (8, 2, 3), (9, 3, 0), (11, 3, 1), (12, 3, 2), (14, 3, 3))
X_LATE = ((12, 1, 2), (14, 1, 3))


def pick(index, pairs, default=0):
    value = jnp.int32(default)
    for key, item in pairs:
        value = jnp.where(index == key, jnp.int32(item), value)
    return value


def kernel(x_ref, w1_ref, w2_ref, o_ref, w1s, w1o, w2, xb, cs, co, cr, hb, zp, zf, zb, ob,
           wsem, xxs, xxr, xfs, xbs, xzr, xc0s, xc0r, xc1s, xc1r, xc2s, xc2r, css, crr, hys, hyr, hx0s, hx0r, hx1s, hx1r,
           hc0s, hc0r, hc1s, hc1r, zss, zfr, zbr, oss, orr):
    p, y, a = lax.axis_index("cz"), lax.axis_index("cy"), lax.axis_index("cx")
    core, ax = lax.rem(a, 2), a // 2
    half = w1s.shape[1]
    a_c, a_x = a + 1 - 2 * core, lax.rem(a + 2, 4)
    a_d = lax.rem(a_c + 2, 4)
    low = p < 2
    edge = (p == 0) | (p == 3)
    middle = (p > 0) & (p < 3)
    ypeer, cpeer, xpeer, dpeer = {"cy": 1 - y}, {"cx": a_c}, {"cx": a_x}, {"cx": a_d}
    front = {"cz": jnp.where(low, p + 1, p - 1)}
    back = {"cz": jnp.where(edge, p, jnp.where(low, p - 1, p + 1))}

    def rcopy(src, dst, ss, rs, device):
        return pltpu.make_async_remote_copy(
            src_ref=src, dst_ref=dst, send_sem=ss, recv_sem=rs, device_id=device, device_id_type=MESH)

    def arrived(ref, sem):
        rcopy(ref, ref, oss, sem, cpeer).wait_recv()

    def sent(ref, sem):
        rcopy(ref, ref, sem, orr, cpeer).wait_send()

    def lanes(owner, width):
        return pl.ds(pl.multiple_of(owner * half, 128), width)

    def plane(k):
        return jnp.where(low, k, 3 - k)

    loads = [
        pltpu.make_async_copy(x_ref, xb.at[pl.ds(4 * p, 4), ax, core], wsem.at[0]),
        pltpu.make_async_copy(w1_ref.at[:, lanes(1 - y, half)], w1s, wsem.at[1]),
        pltpu.make_async_copy(w1_ref.at[:, lanes(y, half)], w1o, wsem.at[2]),
        pltpu.make_async_copy(w2_ref, w2, wsem.at[3]),
    ]
    for load in loads:
        load.start()

    barrier = pltpu.get_barrier_semaphore()
    for device in (ypeer, cpeer, xpeer, dpeer, front):
        pl.semaphore_signal(barrier, inc=1, device_id=device, device_id_type=MESH)

    @pl.when(middle)
    def _():
        pl.semaphore_signal(barrier, inc=1, device_id=back, device_id_type=MESH)
        pl.semaphore_wait(barrier, 6)

    @pl.when(edge)
    def _():
        pl.semaphore_wait(barrier, 5)

    def x_front(g):
        pair = xb.at[g, :, core]
        rcopy(pair, pair, xfs, xzr.at[g], front).start()

    def x_back(g):
        pair = xb.at[g, :, core]
        rcopy(pair, pair, xbs, xzr.at[g], back).start()

    def pair_to_core(g):
        pair = xb.at[g, :, core]
        rcopy(pair, pair, xc2s, xc2r.at[g], cpeer).start()

    def own_arrived(j):
        piece = xb.at[4 * p + j, 1 - ax, core]
        arrived(piece, xxr.at[j])
        rcopy(piece, piece, xc1s, xc1r.at[j], cpeer).start()
        x_front(4 * p + j)

        @pl.when(middle & (j < 2))
        def _():
            x_back(4 * p + j)

    loads[0].wait()
    for j in range(4):
        piece = xb.at[4 * p + j, ax, core]
        rcopy(piece, piece, xc0s, xc0r.at[j], cpeer).start()
        rcopy(piece, piece, xxs, xxr.at[j], xpeer).start()
    loads[1].wait()

    def chunk(i):
        place = i // 4
        base = jnp.where(edge, pick(place, tuple(enumerate(EDGE))), pick(place, tuple(enumerate(MIDDLE))))
        return 8 * plane(base // 2) + 4 * lax.rem(base, 2) + lax.rem(i, 4)

    def chunk1(i):
        turn = i // 2
        first = 8 * p + 2 * lax.rem(i, 2) + turn + ax - 2 * turn * ax
        return jnp.where(i < 4, first, chunk(i))

    def layer1(n):
        g, h = n // 2, lax.rem(n, 2)
        j = lax.rem(g, 4)
        own = g // 4 == p
        theirs = xb.at[g, :, 1 - core]

        @pl.when(own & (h == ax))
        def _():
            arrived(xb.at[g, h, 1 - core], xc0r.at[j])

        @pl.when(own & (h != ax))
        def _():
            arrived(xb.at[g, h, 1 - core], xc1r.at[j])

        @pl.when((g // 4 != p) & (h == 0))
        def _():
            arrived(theirs, xc2r.at[g])

        xv = xb[g, h].reshape(ROWS, xb.shape[4])
        cs[n] = jnp.dot(xv, w1s[...], preferred_element_type=jnp.float32)
        rcopy(cs.at[n], cr.at[n], css, crr.at[n], ypeer).start()

        @pl.when(n == 8 * p + ax)
        def _():
            loads[2].wait()

        co[n] = jnp.dot(xv, w1o[...], preferred_element_type=jnp.float32)

    def h_piece(n, owner, width):
        return hb.at[n, :, lanes(owner, width)]

    def activation(n):
        arrived(cr.at[n], crr.at[n])
        c = (co[n] + cr[n]).astype(jnp.bfloat16).astype(jnp.float32)
        hb[n, :, lanes(2 * a + y, half)] = jax.nn.gelu(c, approximate=True).astype(jnp.bfloat16)
        piece = h_piece(n, 2 * a + y, half)
        rcopy(piece, piece, hys, hyr.at[n], ypeer).start()
        rcopy(piece, piece, hx0s, hx0r.at[n], xpeer).start()

    def pass_y(n):
        piece = h_piece(n, 2 * a + 1 - y, half)
        arrived(piece, hyr.at[n])
        rcopy(piece, piece, hx1s, hx1r.at[n], xpeer).start()
        piece = h_piece(n, 2 * a, 2 * half)
        rcopy(piece, piece, hc0s, hc0r.at[n], cpeer).start()

    def pass_x(n):
        arrived(h_piece(n, 2 * a_x + y, half), hx0r.at[n])
        arrived(h_piece(n, 2 * a_x + 1 - y, half), hx1r.at[n])
        piece = h_piece(n, 2 * a_x, 2 * half)
        rcopy(piece, piece, hc1s, hc1r.at[n], cpeer).start()

    def layer2(n):
        arrived(h_piece(n, 2 * a_c, 2 * half), hc0r.at[n])
        arrived(h_piece(n, 2 * a_d, 2 * half), hc1r.at[n])
        zp[n] = jnp.dot(hb[n], w2[...], preferred_element_type=jnp.float32)

    def from_front(n):
        arrived(zf.at[n], zfr.at[n])
        zp[n] = zp[n] + zf[n]

    def from_back(n):
        arrived(zb.at[n], zbr.at[n])
        zp[n] = zp[n] + zb[n]

    def finish(i):
        n = 8 * p + i
        from_front(n)

        @pl.when(middle)
        def _():
            from_back(n)

        ob[i] = zp[n].astype(jnp.bfloat16).reshape(ob.shape[1:])
        j, h = i // 2, lax.rem(i, 2)
        place = o_ref.at[j, :, lanes(a, half)]

        @pl.when(h == ax)
        def _():
            pltpu.make_async_copy(ob.at[i, core], place, orr).start()
            rcopy(ob.at[i, 1 - core], place, oss, orr, cpeer).start()

        @pl.when(h != ax)
        def _():
            rcopy(ob.at[i, core], place, oss, orr, xpeer).start()
            rcopy(ob.at[i, 1 - core], place, oss, orr, dpeer).start()

    def step(s, carry):
        @pl.when(s < CHUNKS)
        def _():
            layer1(chunk1(s))

        @pl.when((s >= LH) & (s < CHUNKS + LH))
        def _():
            activation(chunk1(s - LH))

        @pl.when(s == 1)
        def _():
            own_arrived(0)

        @pl.when((s >= 1) & (s < 4))
        def _():
            own_arrived(s)

        group = pick(s, [(at, 4 * k + j) for at, k, j in X_EDGE], -1)

        @pl.when(edge & (group >= 0))
        def _():
            g = 4 * plane(group // 4) + lax.rem(group, 4)
            arrived(xb.at[g, :, core], xzr.at[g])
            pair_to_core(g)

        group_b = pick(s, [(at, 4 * k + j) for at, k, j in X_BACK], -1)

        @pl.when(middle & (group_b >= 0))
        def _():
            g = 4 * plane(group_b // 4) + lax.rem(group_b, 4)
            arrived(xb.at[g, :, core], xzr.at[g])
            x_front(g)
            pair_to_core(g)

        group_f = pick(s, [(at, 4 * k + j) for at, k, j in X_FRONT], -1)

        @pl.when(middle & (group_f >= 0))
        def _():
            g = 4 * plane(group_f // 4) + lax.rem(group_f, 4)
            arrived(xb.at[g, :, core], xzr.at[g])
            x_back(g)
            pair_to_core(g)

        late = pick(s, [(at, j) for at, _, j in X_LATE], -1)

        @pl.when(middle & (late >= 0))
        def _():
            x_back(4 * p + late)

        t = s - L2

        @pl.when(t == 0)
        def _():
            loads[3].wait()

        @pl.when((t >= 0) & (t < CHUNKS))
        def _():
            layer2(chunk(t))

        def z_front(n, to):
            rcopy(zp.at[n], to.at[n], zss, (zbr if to is zb else zfr).at[n], front).start()

        @pl.when(edge & (t >= 4) & (t < 28))
        def _():
            z_front(chunk(t), zb)

        @pl.when(middle & (((t >= 12) & (t < 16)) | ((t >= 24) & (t < 28))))
        def _():
            n = chunk(t)
            from_back(n)
            z_front(n, zf)

        @pl.when(middle & (t >= 16 + LZ) & (t < 24 + LZ))
        def _():
            n = chunk(t - LZ)
            from_back(n)
            z_front(n, zf)

        @pl.when(middle & (t >= 16 + 2 * LZ) & (t < 24 + 2 * LZ))
        def _():
            n = chunk(t - 12 - 2 * LZ)
            from_front(n)
            rcopy(zp.at[n], zf.at[n], zss, zfr.at[n], back).start()

        @pl.when((s >= LF) & (s < CHUNKS + LF))
        def _():
            pass_y(chunk1(s - LF))

        @pl.when((s >= LC) & (s < CHUNKS + LC))
        def _():
            pass_x(chunk(s - LC))

        @pl.when(t >= 24)
        def _():
            finish(t - 24)

        return carry

    lax.fori_loop(0, CHUNKS + L2, step, 0)

    arrived(o_ref, orr)
    sent(ob.at[pl.ds(0, 6)], oss)
    sent(cs, css)
    for sem in (hys, hx0s, hx1s):
        sent(hb.at[:, :, pl.ds(0, half)], sem)
    for sem in (hc0s, hc1s):
        sent(hb.at[:, :, pl.ds(0, 2 * half)], sem)
    sent(zp.at[pl.ds(0, 24)], zss)
    for sem in (xxs, xc0s, xc1s):
        sent(xb.at[pl.ds(0, 4), 0, 0], sem)
    sent(xb.at[pl.ds(0, 12), :, 0], xc2s)

    @pl.when(edge)
    def _():
        sent(xb.at[pl.ds(0, 4), :, 0], xfs)

    @pl.when(middle)
    def _():
        sent(xb.at[pl.ds(0, 8), :, 0], xfs)
        sent(xb.at[pl.ds(0, 12), :, 0], xbs)


def solution(mesh):
    def body(x, w1, w2):
        r, d = x.shape
        k1, n1 = w1.shape
        k2, n2 = w2.shape
        half = n1 // 2
        f32, bf16 = jnp.float32, jnp.bfloat16
        dma = pltpu.SemaphoreType.DMA
        one, four, groups, chunks = dma(()), dma((4,)), dma((16,)), dma((CHUNKS,))
        out = pl.pallas_call(
            kernel,
            out_shape=jax.ShapeDtypeStruct((4, r // 4, d), bf16),
            in_specs=[pl.BlockSpec(memory_space=pl.ANY)] * 3,
            out_specs=pl.BlockSpec(memory_space=pl.ANY),
            scratch_shapes=[
                pltpu.VMEM((k1, half), bf16),
                pltpu.VMEM((k1, half), bf16),
                pltpu.VMEM((k2, n2), bf16),
                pltpu.VMEM((16, 2, 2, 16, d), bf16),
                pltpu.VMEM((CHUNKS, ROWS, half), f32),
                pltpu.VMEM((CHUNKS, ROWS, half), f32),
                pltpu.VMEM((CHUNKS, ROWS, half), f32),
                pltpu.VMEM((CHUNKS, ROWS, k2), bf16),
                pltpu.VMEM((CHUNKS, ROWS, n2), f32),
                pltpu.VMEM((CHUNKS, ROWS, n2), f32),
                pltpu.VMEM((CHUNKS, ROWS, n2), f32),
                pltpu.VMEM((8, 2, 16, n2), bf16),
                four,
                one, four,
                one, one, groups,
                one, four, one, four, one, groups,
                one, chunks,
                one, chunks,
                one, chunks,
                one, chunks,
                one, chunks,
                one, chunks,
                one, chunks, chunks,
                one, one,
            ],
            compiler_params=pltpu.CompilerParams(
                collective_id=0, has_side_effects=True, vmem_limit_bytes=60 * 1024 * 1024),
            name="mlp",
        )(x.reshape(4, r // 4, d), w1, w2)
        return out.reshape(r, d)

    return jax.shard_map(
        body,
        mesh=mesh,
        in_specs=(P(("cx", "cz"), "cy"), P("cy", ("cz", "cx")), P("cz", ("cy", "cx"))),
        out_specs=P(("cx", "cz"), "cy"),
        check_vma=False,
    )
```

```python
import jax
import jax.numpy as jnp
from jax import lax
from jax.experimental import pallas as pl
from jax.experimental.pallas import tpu as pltpu
from jax.sharding import PartitionSpec as P

MESH = pl.DeviceIdType.MESH
CHUNKS, ROWS = 32, 32
TURNS = 20
LH, LF, LC, L2 = 2, 4, 5, 6
EDGE = (0, 2, 4, 6, 7, 5, 3, 1)
MIDDLE = (2, 0, 1, 4, 6, 7, 5, 3)
X_EDGE = tuple((3 + e, k, j) for e, (k, j) in enumerate(
    ((1, 0), (1, 1), (2, 0), (2, 1), (3, 0), (3, 1), (3, 2), (3, 3), (2, 2), (2, 3), (1, 2), (1, 3))))
X_BACK = tuple((3 + j, 0, j) for j in range(4))
X_FRONT = tuple((3 + e, 2 + e // 4, e % 4) for e in range(8))
X_LATE = ((10, 1, 2), (11, 1, 3))


def pick(index, pairs, default=0):
    value = jnp.int32(default)
    for key, item in pairs:
        value = jnp.where(index == key, jnp.int32(item), value)
    return value


def kernel(x_ref, w1_ref, w2_ref, o_ref, w1s, w1o, w2, xb, cs, co, cr, hb, zp, zf, zb, ob,
           wsem, xxs, xxr, xfs, xbs, xzr, xc0s, xc0r, xc1s, xc1r, xc2s, xc2r, css, crr, hys, hyr, hxs, hxr,
           hcs, hcr, zss, zfr, zbr, oss, orr):
    p, y, a = lax.axis_index("cz"), lax.axis_index("cy"), lax.axis_index("cx")
    core, ax = lax.rem(a, 2), a // 2
    half = w1s.shape[1]
    a_c, a_x = a + 1 - 2 * core, lax.rem(a + 2, 4)
    a_d = lax.rem(a_c + 2, 4)
    low = p < 2
    edge = (p == 0) | (p == 3)
    middle = (p > 0) & (p < 3)
    ypeer, cpeer, xpeer, dpeer = {"cy": 1 - y}, {"cx": a_c}, {"cx": a_x}, {"cx": a_d}
    front = {"cz": jnp.where(low, p + 1, p - 1)}
    back = {"cz": jnp.where(edge, p, jnp.where(low, p - 1, p + 1))}

    def rcopy(src, dst, ss, rs, device):
        return pltpu.make_async_remote_copy(
            src_ref=src, dst_ref=dst, send_sem=ss, recv_sem=rs, device_id=device, device_id_type=MESH)

    def arrived(ref, sem):
        rcopy(ref, ref, oss, sem, cpeer).wait_recv()

    def sent(ref, sem):
        rcopy(ref, ref, sem, orr, cpeer).wait_send()

    def lanes(owner, width):
        return pl.ds(pl.multiple_of(owner * half, 128), width)

    def plane(k):
        return jnp.where(low, k, 3 - k)

    loads = [
        pltpu.make_async_copy(x_ref, xb.at[pl.ds(4 * p, 4), ax, core], wsem.at[0]),
        pltpu.make_async_copy(w1_ref.at[:, lanes(1 - y, half)], w1s, wsem.at[1]),
        pltpu.make_async_copy(w1_ref.at[:, lanes(y, half)], w1o, wsem.at[2]),
        pltpu.make_async_copy(w2_ref, w2, wsem.at[3]),
    ]
    for load in loads:
        load.start()

    barrier = pltpu.get_barrier_semaphore()
    for device in (ypeer, cpeer, xpeer, dpeer, front):
        pl.semaphore_signal(barrier, inc=1, device_id=device, device_id_type=MESH)

    @pl.when(middle)
    def _():
        pl.semaphore_signal(barrier, inc=1, device_id=back, device_id_type=MESH)
        pl.semaphore_wait(barrier, 6)

    @pl.when(edge)
    def _():
        pl.semaphore_wait(barrier, 5)

    def x_front(g):
        pair = xb.at[g, :, core]
        rcopy(pair, pair, xfs, xzr.at[g], front).start()

    def x_back(g):
        pair = xb.at[g, :, core]
        rcopy(pair, pair, xbs, xzr.at[g], back).start()

    def pair_to_core(g):
        pair = xb.at[g, :, core]
        rcopy(pair, pair, xc2s, xc2r.at[g], cpeer).start()

    def own_arrived(j):
        piece = xb.at[4 * p + j, 1 - ax, core]
        arrived(piece, xxr.at[j])
        rcopy(piece, piece, xc1s, xc1r.at[j], cpeer).start()
        x_front(4 * p + j)

        @pl.when(middle & (j < 2))
        def _():
            x_back(4 * p + j)

    loads[0].wait()
    for j in range(4):
        piece = xb.at[4 * p + j, ax, core]
        rcopy(piece, piece, xc0s, xc0r.at[j], cpeer).start()
        rcopy(piece, piece, xxs, xxr.at[j], xpeer).start()
    loads[1].wait()

    def chunk(u):
        place = (u - 2) // 2
        base = jnp.where(edge, pick(place, tuple(enumerate(EDGE))), pick(place, tuple(enumerate(MIDDLE))))
        other = 8 * plane(base // 2) + 4 * lax.rem(base, 2) + 2 * lax.rem(u, 2)
        return jnp.where(u < 4, 8 * p + u, jnp.where(u < 16, other, 8 * p + u - 12))

    def chunk1(u):
        turn = u // 2
        first = 8 * p + 2 * lax.rem(u, 2) + turn + ax - 2 * turn * ax
        return jnp.where(u < 4, first, chunk(u))

    def rows_of(ref, n, count):
        return ref.at[pl.ds(n, count)]

    def product(xv, w, count):
        z = jnp.dot(xv.reshape(count * ROWS, xv.shape[-1]), w[...], preferred_element_type=jnp.float32)
        return z.reshape(count, ROWS, z.shape[1])

    def layer1(n, count, start):
        g, h = n // 2, lax.rem(n, 2)
        if count == 2:
            arrived(xb.at[g, :, 1 - core], xc2r.at[g])
            xv = xb[g]
        else:
            j = lax.rem(g, 4)

            @pl.when(h == ax)
            def _():
                arrived(xb.at[g, h, 1 - core], xc0r.at[j])

            @pl.when(h != ax)
            def _():
                arrived(xb.at[g, h, 1 - core], xc1r.at[j])

            xv = xb[g, h]
        cs[pl.ds(n, count)] = product(xv, w1s, count)
        rcopy(rows_of(cs, n, count), rows_of(cr, n, count), css, crr.at[n], ypeer).start()
        if count == 1:
            @pl.when(start)
            def _():
                loads[2].wait()

        co[pl.ds(n, count)] = product(xv, w1o, count)

    def h_piece(n, count, owner, width):
        return hb.at[pl.ds(n, count), :, lanes(owner, width)]

    def activation(n, count):
        arrived(rows_of(cr, n, count), crr.at[n])
        c = (co[pl.ds(n, count)] + cr[pl.ds(n, count)]).astype(jnp.bfloat16).astype(jnp.float32)
        h = jax.nn.gelu(c, approximate=True).astype(jnp.bfloat16)
        hb[pl.ds(n, count), :, lanes(2 * a + y, half)] = h
        piece = h_piece(n, count, 2 * a + y, half)
        rcopy(piece, piece, hys, hyr.at[n], ypeer).start()
        rcopy(piece, piece, hxs, hxr.at[n], xpeer).start()

    def pass_y(n, count):
        piece = h_piece(n, count, 2 * a + 1 - y, half)
        arrived(piece, hyr.at[n])
        rcopy(piece, piece, hxs, hxr.at[n], xpeer).start()
        piece = h_piece(n, count, 2 * a, 2 * half)
        rcopy(piece, piece, hcs, hcr.at[n], cpeer).start()

    def pass_x(n, count):
        piece = h_piece(n, count, 2 * a_x, 2 * half)
        arrived(piece, hxr.at[n])
        rcopy(piece, piece, hcs, hcr.at[n], cpeer).start()

    def layer2(n, count):
        arrived(h_piece(n, count, 0, 4 * half), hcr.at[n])
        zp[pl.ds(n, count)] = product(hb[pl.ds(n, count)], w2, count)

    def z_send(n, to, sems, device):
        rcopy(rows_of(zp, n, 2), rows_of(to, n, 2), zss, sems.at[n], device).start()

    def add(n, count, ref):
        zp[pl.ds(n, count)] = zp[pl.ds(n, count)] + ref[pl.ds(n, count)]

    def out_piece(i, c, j, device):
        rcopy(ob.at[i, c], o_ref.at[j, :, lanes(a, half)], oss, orr, device).start()

    def out_own(i, j):
        pltpu.make_async_copy(ob.at[i, core], o_ref.at[j, :, lanes(a, half)], orr).start()
        out_piece(i, 1 - core, j, cpeer)

    def out_other(i, j):
        out_piece(i, core, j, xpeer)
        out_piece(i, 1 - core, j, dpeer)

    def partials_arrived(n):
        arrived(rows_of(zf, n, 2), zfr.at[n])

        @pl.when(middle)
        def _():
            arrived(rows_of(zb, n, 2), zbr.at[n])

    def finish(i, count):
        n = 8 * p + i
        add(n, count, zf)

        @pl.when(middle)
        def _():
            add(n, count, zb)

        ob[pl.ds(i, count)] = zp[pl.ds(n, count)].astype(jnp.bfloat16).reshape((count,) + ob.shape[1:])

    def step(s, carry):
        def each(u, event):
            @pl.when(((u >= 0) & (u < 4)) | ((u >= 16) & (u < TURNS)))
            def _():
                event(u, 1)

            @pl.when((u >= 4) & (u < 16))
            def _():
                event(u, 2)

        each(s, lambda u, count: layer1(chunk1(u), count, s == 0))
        each(s - LH, lambda u, count: activation(chunk1(u), count))
        each(s - LF, lambda u, count: pass_y(chunk1(u), count))

        @pl.when(s == 1)
        def _():
            own_arrived(0)

        @pl.when((s >= 1) & (s < 4))
        def _():
            own_arrived(s)

        group = pick(s, [(at, 4 * k + j) for at, k, j in X_EDGE], -1)

        @pl.when(edge & (group >= 0))
        def _():
            g = 4 * plane(group // 4) + lax.rem(group, 4)
            arrived(xb.at[g, :, core], xzr.at[g])
            pair_to_core(g)

        group_b = pick(s, [(at, 4 * k + j) for at, k, j in X_BACK], -1)

        @pl.when(middle & (group_b >= 0))
        def _():
            g = 4 * plane(group_b // 4) + lax.rem(group_b, 4)
            arrived(xb.at[g, :, core], xzr.at[g])
            x_front(g)
            pair_to_core(g)

        group_f = pick(s, [(at, 4 * k + j) for at, k, j in X_FRONT], -1)

        @pl.when(middle & (group_f >= 0))
        def _():
            g = 4 * plane(group_f // 4) + lax.rem(group_f, 4)
            arrived(xb.at[g, :, core], xzr.at[g])
            x_back(g)
            pair_to_core(g)

        late = pick(s, [(at, j) for at, _, j in X_LATE], -1)

        @pl.when(middle & (late >= 0))
        def _():
            x_back(4 * p + late)

        t = s - L2

        @pl.when(t == 0)
        def _():
            loads[3].wait()

        each(t, lambda u, count: layer2(chunk(u), count))

        @pl.when(edge & (t >= 4) & (t < 16))
        def _():
            z_send(chunk(t), zb, zbr, front)

        @pl.when(middle & (t >= 8) & (t < 16))
        def _():
            n = chunk(t)
            arrived(rows_of(zb, n, 2), zbr.at[n])
            add(n, 2, zb)
            z_send(n, zf, zfr, front)

        @pl.when(middle & (t >= 12) & (t < 16))
        def _():
            n = 8 * plane(0) + 2 * (t - 12)
            arrived(rows_of(zf, n, 2), zfr.at[n])
            add(n, 2, zf)
            z_send(n, zf, zfr, back)

        each(s - LC, lambda u, count: pass_x(chunk(u), count))

        @pl.when((t >= 15) & (t < 17))
        def _():
            j = t - 15
            partials_arrived(8 * p + 2 * j)
            finish(2 * j, 2)
            out_own(2 * j + ax, j)
            out_other(2 * j + 1 - ax, j)

        @pl.when(t >= 16)
        def _():
            i = t - 12
            j, h = i // 2, lax.rem(i, 2)

            @pl.when(h == 0)
            def _():
                partials_arrived(8 * p + i)

            finish(i, 1)

            @pl.when(h == ax)
            def _():
                out_own(i, j)

            @pl.when(h != ax)
            def _():
                out_other(i, j)

        return carry

    lax.fori_loop(0, TURNS + L2, step, 0)

    arrived(o_ref, orr)
    sent(ob.at[pl.ds(0, 6)], oss)
    sent(cs, css)
    for sem, width in ((hys, half), (hxs, 2 * half), (hcs, 4 * half)):
        sent(hb.at[:, :, pl.ds(0, width)], sem)
    sent(zp.at[pl.ds(0, 24)], zss)
    for sem in (xxs, xc0s, xc1s):
        sent(xb.at[pl.ds(0, 4), 0, 0], sem)
    sent(xb.at[pl.ds(0, 12), :, 0], xc2s)

    @pl.when(edge)
    def _():
        sent(xb.at[pl.ds(0, 4), :, 0], xfs)

    @pl.when(middle)
    def _():
        sent(xb.at[pl.ds(0, 8), :, 0], xfs)
        sent(xb.at[pl.ds(0, 12), :, 0], xbs)


def solution(mesh):
    def body(x, w1, w2):
        r, d = x.shape
        k1, n1 = w1.shape
        k2, n2 = w2.shape
        half = n1 // 2
        f32, bf16 = jnp.float32, jnp.bfloat16
        dma = pltpu.SemaphoreType.DMA
        one, four, groups, chunks = dma(()), dma((4,)), dma((16,)), dma((CHUNKS,))
        out = pl.pallas_call(
            kernel,
            out_shape=jax.ShapeDtypeStruct((4, r // 4, d), bf16),
            in_specs=[pl.BlockSpec(memory_space=pl.ANY)] * 3,
            out_specs=pl.BlockSpec(memory_space=pl.ANY),
            scratch_shapes=[
                pltpu.VMEM((k1, half), bf16),
                pltpu.VMEM((k1, half), bf16),
                pltpu.VMEM((k2, n2), bf16),
                pltpu.VMEM((16, 2, 2, 16, d), bf16),
                pltpu.VMEM((CHUNKS, ROWS, half), f32),
                pltpu.VMEM((CHUNKS, ROWS, half), f32),
                pltpu.VMEM((CHUNKS, ROWS, half), f32),
                pltpu.VMEM((CHUNKS, ROWS, k2), bf16),
                pltpu.VMEM((CHUNKS, ROWS, n2), f32),
                pltpu.VMEM((CHUNKS, ROWS, n2), f32),
                pltpu.VMEM((CHUNKS, ROWS, n2), f32),
                pltpu.VMEM((8, 2, 16, n2), bf16),
                four,
                one, four,
                one, one, groups,
                one, four, one, four, one, groups,
                one, chunks,
                one, chunks,
                one, chunks,
                one, chunks,
                one, chunks, chunks,
                one, one,
            ],
            compiler_params=pltpu.CompilerParams(
                collective_id=0, has_side_effects=True, vmem_limit_bytes=60 * 1024 * 1024),
            name="mlp",
        )(x.reshape(4, r // 4, d), w1, w2)
        return out.reshape(r, d)

    return jax.shard_map(
        body,
        mesh=mesh,
        in_specs=(P(("cx", "cz"), "cy"), P("cy", ("cz", "cx")), P("cz", ("cy", "cx"))),
        out_specs=P(("cx", "cz"), "cy"),
        check_vma=False,
    )
```

```python
import jax
import jax.numpy as jnp
from jax import lax
from jax.experimental import pallas as pl
from jax.experimental.pallas import tpu as pltpu
from jax.sharding import PartitionSpec as P

MESH = pl.DeviceIdType.MESH
CHUNKS, ROWS = 32, 32
TURNS = 20
LH, LF, LC, L2 = 1, 3, 5, 6
EDGE = (0, 2, 4, 6, 7, 5, 3, 1)
MIDDLE = (2, 0, 1, 4, 6, 7, 5, 3)
X_EDGE = tuple((3 + e, k, j) for e, (k, j) in enumerate(
    ((1, 0), (1, 1), (2, 0), (2, 1), (3, 0), (3, 1), (3, 2), (3, 3), (2, 2), (2, 3), (1, 2), (1, 3))))
X_BACK = tuple((3 + j, 0, j) for j in range(4))
X_FRONT = tuple((3 + e, 2 + e // 4, e % 4) for e in range(8))
X_LATE = ((10, 1, 2), (11, 1, 3))


def pick(index, pairs, default=0):
    value = jnp.int32(default)
    for key, item in pairs:
        value = jnp.where(index == key, jnp.int32(item), value)
    return value


def kernel(x_ref, w1_ref, w2_ref, o_ref, w1s, w1o, w2, xb, cs, co, cr, hb, zp, zf, zb, ob,
           wsem, xxs, xxr, xfs, xbs, xzr, xc0s, xc0r, xc1s, xc1r, xc2s, xc2r, css, crr, hys, hyr, hxs, hxr,
           hcs, hcr, zss, zfr, zbr, oss, orr):
    p, y, a = lax.axis_index("cz"), lax.axis_index("cy"), lax.axis_index("cx")
    core, ax = lax.rem(a, 2), a // 2
    half = w1s.shape[1]
    a_c, a_x = a + 1 - 2 * core, lax.rem(a + 2, 4)
    a_d = lax.rem(a_c + 2, 4)
    low = p < 2
    edge = (p == 0) | (p == 3)
    middle = (p > 0) & (p < 3)
    ypeer, cpeer, xpeer, dpeer = {"cy": 1 - y}, {"cx": a_c}, {"cx": a_x}, {"cx": a_d}
    front = {"cz": jnp.where(low, p + 1, p - 1)}
    back = {"cz": jnp.where(edge, p, jnp.where(low, p - 1, p + 1))}

    def rcopy(src, dst, ss, rs, device):
        return pltpu.make_async_remote_copy(
            src_ref=src, dst_ref=dst, send_sem=ss, recv_sem=rs, device_id=device, device_id_type=MESH)

    def arrived(ref, sem):
        rcopy(ref, ref, oss, sem, cpeer).wait_recv()

    def sent(ref, sem):
        rcopy(ref, ref, sem, orr, cpeer).wait_send()

    def lanes(owner, width):
        return pl.ds(pl.multiple_of(owner * half, 128), width)

    def plane(k):
        return jnp.where(low, k, 3 - k)

    loads = [
        pltpu.make_async_copy(x_ref, xb.at[pl.ds(4 * p, 4), ax, core], wsem.at[0]),
        pltpu.make_async_copy(w1_ref.at[:, lanes(1 - y, half)], w1s, wsem.at[1]),
        pltpu.make_async_copy(w1_ref.at[:, lanes(y, half)], w1o, wsem.at[2]),
        pltpu.make_async_copy(w2_ref, w2, wsem.at[3]),
    ]
    for load in loads:
        load.start()

    barrier = pltpu.get_barrier_semaphore()
    for device in (ypeer, cpeer, xpeer, dpeer, front):
        pl.semaphore_signal(barrier, inc=1, device_id=device, device_id_type=MESH)

    @pl.when(middle)
    def _():
        pl.semaphore_signal(barrier, inc=1, device_id=back, device_id_type=MESH)
        pl.semaphore_wait(barrier, 6)

    @pl.when(edge)
    def _():
        pl.semaphore_wait(barrier, 5)

    def x_front(g):
        pair = xb.at[g, :, core]
        rcopy(pair, pair, xfs, xzr.at[g], front).start()

    def x_back(g):
        pair = xb.at[g, :, core]
        rcopy(pair, pair, xbs, xzr.at[g], back).start()

    def pair_to_core(g):
        pair = xb.at[g, :, core]
        rcopy(pair, pair, xc2s, xc2r.at[g], cpeer).start()

    def own_arrived(j):
        piece = xb.at[4 * p + j, 1 - ax, core]
        arrived(piece, xxr.at[j])
        rcopy(piece, piece, xc1s, xc1r.at[j], cpeer).start()
        x_front(4 * p + j)

        @pl.when(middle & (j < 2))
        def _():
            x_back(4 * p + j)

    loads[0].wait()
    for j in range(4):
        piece = xb.at[4 * p + j, ax, core]
        rcopy(piece, piece, xc0s, xc0r.at[j], cpeer).start()
        rcopy(piece, piece, xxs, xxr.at[j], xpeer).start()
    loads[1].wait()

    def chunk(u):
        place = (u - 2) // 2
        base = jnp.where(edge, pick(place, tuple(enumerate(EDGE))), pick(place, tuple(enumerate(MIDDLE))))
        other = 8 * plane(base // 2) + 4 * lax.rem(base, 2) + 2 * lax.rem(u, 2)
        return jnp.where(u < 4, 8 * p + u, jnp.where(u < 16, other, 8 * p + u - 12))

    def chunk1(u):
        turn = u // 2
        first = 8 * p + 2 * lax.rem(u, 2) + turn + ax - 2 * turn * ax
        return jnp.where(u < 4, first, chunk(u))

    def rows_of(ref, n, count):
        return ref.at[pl.ds(n, count)]

    def product(xv, w, count):
        z = jnp.dot(xv.reshape(count * ROWS, xv.shape[-1]), w[...], preferred_element_type=jnp.float32)
        return z.reshape(count, ROWS, z.shape[1])

    def layer1(n, count, start):
        g, h = n // 2, lax.rem(n, 2)
        if count == 2:
            arrived(xb.at[g, :, 1 - core], xc2r.at[g])
            xv = xb[g]
        else:
            j = lax.rem(g, 4)

            @pl.when(h == ax)
            def _():
                arrived(xb.at[g, h, 1 - core], xc0r.at[j])

            @pl.when(h != ax)
            def _():
                arrived(xb.at[g, h, 1 - core], xc1r.at[j])

            xv = xb[g, h]
        cs[pl.ds(n, count)] = product(xv, w1s, count)
        rcopy(rows_of(cs, n, count), rows_of(cr, n, count), css, crr.at[n], ypeer).start()
        if count == 1:
            @pl.when(start)
            def _():
                loads[2].wait()

        co[pl.ds(n, count)] = product(xv, w1o, count)

    def h_piece(n, count, owner, width):
        return hb.at[pl.ds(n, count), :, lanes(owner, width)]

    def activation(n, count):
        arrived(rows_of(cr, n, count), crr.at[n])
        c = (co[pl.ds(n, count)] + cr[pl.ds(n, count)]).astype(jnp.bfloat16).astype(jnp.float32)
        h = jax.nn.gelu(c, approximate=True).astype(jnp.bfloat16)
        hb[pl.ds(n, count), :, lanes(2 * a + y, half)] = h
        piece = h_piece(n, count, 2 * a + y, half)
        rcopy(piece, piece, hys, hyr.at[n], ypeer).start()
        rcopy(piece, piece, hxs, hxr.at[n], xpeer).start()

    def pass_y(n, count):
        piece = h_piece(n, count, 2 * a + 1 - y, half)
        arrived(piece, hyr.at[n])
        rcopy(piece, piece, hxs, hxr.at[n], xpeer).start()
        piece = h_piece(n, count, 2 * a, 2 * half)
        rcopy(piece, piece, hcs, hcr.at[n], cpeer).start()

    def pass_x(n, count):
        piece = h_piece(n, count, 2 * a_x, 2 * half)
        arrived(piece, hxr.at[n])
        rcopy(piece, piece, hcs, hcr.at[n], cpeer).start()

    def layer2(n, count):
        arrived(h_piece(n, count, 0, 4 * half), hcr.at[n])
        zp[pl.ds(n, count)] = product(hb[pl.ds(n, count)], w2, count)

    def z_send(n, to, sems, device):
        rcopy(rows_of(zp, n, 2), rows_of(to, n, 2), zss, sems.at[n], device).start()

    def add(n, count, ref):
        zp[pl.ds(n, count)] = zp[pl.ds(n, count)] + ref[pl.ds(n, count)]

    def out_piece(i, c, j, device):
        rcopy(ob.at[i, c], o_ref.at[j, :, lanes(a, half)], oss, orr, device).start()

    def out_own(i, j):
        pltpu.make_async_copy(ob.at[i, core], o_ref.at[j, :, lanes(a, half)], orr).start()
        out_piece(i, 1 - core, j, cpeer)

    def out_other(i, j):
        out_piece(i, core, j, xpeer)
        out_piece(i, 1 - core, j, dpeer)

    def partials_arrived(n):
        arrived(rows_of(zf, n, 2), zfr.at[n])

        @pl.when(middle)
        def _():
            arrived(rows_of(zb, n, 2), zbr.at[n])

    def finish(i, count):
        n = 8 * p + i
        add(n, count, zf)

        @pl.when(middle)
        def _():
            add(n, count, zb)

        ob[pl.ds(i, count)] = zp[pl.ds(n, count)].astype(jnp.bfloat16).reshape((count,) + ob.shape[1:])

    def step(s, carry):
        def each(u, event):
            @pl.when(((u >= 0) & (u < 4)) | ((u >= 16) & (u < TURNS)))
            def _():
                event(u, 1)

            @pl.when((u >= 4) & (u < 16))
            def _():
                event(u, 2)

        each(s, lambda u, count: layer1(chunk1(u), count, s == 0))
        each(s - LF, lambda u, count: pass_y(chunk1(u), count))

        @pl.when(s == 1)
        def _():
            own_arrived(0)

        @pl.when((s >= 1) & (s < 4))
        def _():
            own_arrived(s)

        group = pick(s, [(at, 4 * k + j) for at, k, j in X_EDGE], -1)

        @pl.when(edge & (group >= 0))
        def _():
            g = 4 * plane(group // 4) + lax.rem(group, 4)
            arrived(xb.at[g, :, core], xzr.at[g])
            pair_to_core(g)

        group_b = pick(s, [(at, 4 * k + j) for at, k, j in X_BACK], -1)

        @pl.when(middle & (group_b >= 0))
        def _():
            g = 4 * plane(group_b // 4) + lax.rem(group_b, 4)
            arrived(xb.at[g, :, core], xzr.at[g])
            x_front(g)
            pair_to_core(g)

        group_f = pick(s, [(at, 4 * k + j) for at, k, j in X_FRONT], -1)

        @pl.when(middle & (group_f >= 0))
        def _():
            g = 4 * plane(group_f // 4) + lax.rem(group_f, 4)
            arrived(xb.at[g, :, core], xzr.at[g])
            x_back(g)
            pair_to_core(g)

        late = pick(s, [(at, j) for at, _, j in X_LATE], -1)

        @pl.when(middle & (late >= 0))
        def _():
            x_back(4 * p + late)

        each(s - LC, lambda u, count: pass_x(chunk(u), count))

        t = s - L2

        @pl.when(t == 0)
        def _():
            loads[3].wait()

        each(t, lambda u, count: layer2(chunk(u), count))

        @pl.when(edge & (t >= 4) & (t < 16))
        def _():
            z_send(chunk(t), zb, zbr, front)

        @pl.when(middle & (t >= 8) & (t < 16))
        def _():
            n = chunk(t)
            arrived(rows_of(zb, n, 2), zbr.at[n])
            add(n, 2, zb)
            z_send(n, zf, zfr, front)

        @pl.when(middle & (t >= 12) & (t < 16))
        def _():
            n = 8 * plane(0) + 2 * (t - 12)
            arrived(rows_of(zf, n, 2), zfr.at[n])
            add(n, 2, zf)
            z_send(n, zf, zfr, back)

        each(s - LH, lambda u, count: activation(chunk1(u), count))

        @pl.when((t >= 15) & (t < 17))
        def _():
            j = t - 15
            partials_arrived(8 * p + 2 * j)
            finish(2 * j, 2)
            out_own(2 * j + ax, j)
            out_other(2 * j + 1 - ax, j)

        @pl.when(t >= 16)
        def _():
            i = t - 12
            j, h = i // 2, lax.rem(i, 2)

            @pl.when(h == 0)
            def _():
                partials_arrived(8 * p + i)

            finish(i, 1)

            @pl.when(h == ax)
            def _():
                out_own(i, j)

            @pl.when(h != ax)
            def _():
                out_other(i, j)

        return carry

    lax.fori_loop(0, TURNS + L2, step, 0)

    arrived(o_ref, orr)
    sent(ob.at[pl.ds(0, 6)], oss)
    sent(cs, css)
    for sem, width in ((hys, half), (hxs, 2 * half), (hcs, 4 * half)):
        sent(hb.at[:, :, pl.ds(0, width)], sem)
    sent(zp.at[pl.ds(0, 24)], zss)
    for sem in (xxs, xc0s, xc1s):
        sent(xb.at[pl.ds(0, 4), 0, 0], sem)
    sent(xb.at[pl.ds(0, 12), :, 0], xc2s)

    @pl.when(edge)
    def _():
        sent(xb.at[pl.ds(0, 4), :, 0], xfs)

    @pl.when(middle)
    def _():
        sent(xb.at[pl.ds(0, 8), :, 0], xfs)
        sent(xb.at[pl.ds(0, 12), :, 0], xbs)


def solution(mesh):
    def body(x, w1, w2):
        r, d = x.shape
        k1, n1 = w1.shape
        k2, n2 = w2.shape
        half = n1 // 2
        f32, bf16 = jnp.float32, jnp.bfloat16
        dma = pltpu.SemaphoreType.DMA
        one, four, groups, chunks = dma(()), dma((4,)), dma((16,)), dma((CHUNKS,))
        out = pl.pallas_call(
            kernel,
            out_shape=jax.ShapeDtypeStruct((4, r // 4, d), bf16),
            in_specs=[pl.BlockSpec(memory_space=pl.ANY)] * 3,
            out_specs=pl.BlockSpec(memory_space=pl.ANY),
            scratch_shapes=[
                pltpu.VMEM((k1, half), bf16),
                pltpu.VMEM((k1, half), bf16),
                pltpu.VMEM((k2, n2), bf16),
                pltpu.VMEM((16, 2, 2, 16, d), bf16),
                pltpu.VMEM((CHUNKS, ROWS, half), f32),
                pltpu.VMEM((CHUNKS, ROWS, half), f32),
                pltpu.VMEM((CHUNKS, ROWS, half), f32),
                pltpu.VMEM((CHUNKS, ROWS, k2), bf16),
                pltpu.VMEM((CHUNKS, ROWS, n2), f32),
                pltpu.VMEM((CHUNKS, ROWS, n2), f32),
                pltpu.VMEM((CHUNKS, ROWS, n2), f32),
                pltpu.VMEM((8, 2, 16, n2), bf16),
                four,
                one, four,
                one, one, groups,
                one, four, one, four, one, groups,
                one, chunks,
                one, chunks,
                one, chunks,
                one, chunks,
                one, chunks, chunks,
                one, one,
            ],
            compiler_params=pltpu.CompilerParams(
                collective_id=0, has_side_effects=True, vmem_limit_bytes=60 * 1024 * 1024),
            name="mlp",
        )(x.reshape(4, r // 4, d), w1, w2)
        return out.reshape(r, d)

    return jax.shard_map(
        body,
        mesh=mesh,
        in_specs=(P(("cx", "cz"), "cy"), P("cy", ("cz", "cx")), P("cz", ("cy", "cx"))),
        out_specs=P(("cx", "cz"), "cy"),
        check_vma=False,
    )
```

```python
import jax
import jax.numpy as jnp
from jax import lax
from jax.experimental import pallas as pl
from jax.experimental.pallas import tpu as pltpu
from jax.sharding import PartitionSpec as P

MESH = pl.DeviceIdType.MESH
CHUNKS, ROWS = 32, 32
LOOPED = 16
LH, LF, LC, L2 = 1, 3, 5, 6
TAIL = (
    "L10 C11 F13 C12 Z10 M16 L11 Z11 F14 C13 H15 L12 Z12 H16 B0 M18 C14 B1 H17 L13 Z13 F15 L14 F16 B2 H18 Z14 H19 C15 "
    "F17 F18 C16 B3 L15 Z15 F19 C17 O0 C18 O1 L16 C19 O2 L18 O3")


EDGE = (0, 2, 4, 6, 7, 5, 3, 1)
MIDDLE = (2, 0, 1, 4, 6, 7, 5, 3)
X_EDGE = tuple((3 + e, k, j) for e, (k, j) in enumerate(
    ((1, 0), (1, 1), (2, 0), (2, 1), (3, 0), (3, 1), (3, 2), (3, 3), (2, 2), (2, 3), (1, 2), (1, 3))))
X_BACK = tuple((3 + j, 0, j) for j in range(4))
X_FRONT = tuple((3 + e, 2 + e // 4, e % 4) for e in range(8))
X_LATE = ((10, 1, 2), (11, 1, 3))


def pick(index, pairs, default=0):
    value = jnp.int32(default)
    for key, item in pairs:
        value = jnp.where(index == key, jnp.int32(item), value)
    return value


def kernel(x_ref, w1_ref, w2_ref, o_ref, w1s, w1o, w2, xb, cs, co, cr, hb, zp, zf, zb, ob,
           wsem, xxs, xxr, xfs, xbs, xzr, xc0s, xc0r, xc1s, xc1r, xc2s, xc2r, css, crr, hys, hyr, hxs, hxr,
           hcs, hcr, zss, zfr, zbr, oss, orr):
    p, y, a = lax.axis_index("cz"), lax.axis_index("cy"), lax.axis_index("cx")
    core, ax = lax.rem(a, 2), a // 2
    half = w1s.shape[1]
    a_c, a_x = a + 1 - 2 * core, lax.rem(a + 2, 4)
    a_d = lax.rem(a_c + 2, 4)
    low = p < 2
    edge = (p == 0) | (p == 3)
    middle = (p > 0) & (p < 3)
    ypeer, cpeer, xpeer, dpeer = {"cy": 1 - y}, {"cx": a_c}, {"cx": a_x}, {"cx": a_d}
    front = {"cz": jnp.where(low, p + 1, p - 1)}
    back = {"cz": jnp.where(edge, p, jnp.where(low, p - 1, p + 1))}

    def rcopy(src, dst, ss, rs, device):
        return pltpu.make_async_remote_copy(
            src_ref=src, dst_ref=dst, send_sem=ss, recv_sem=rs, device_id=device, device_id_type=MESH)

    def arrived(ref, sem):
        rcopy(ref, ref, oss, sem, cpeer).wait_recv()

    def sent(ref, sem):
        rcopy(ref, ref, sem, orr, cpeer).wait_send()

    def lanes(owner, width):
        return pl.ds(pl.multiple_of(owner * half, 128), width)

    def plane(k):
        return jnp.where(low, k, 3 - k)

    loads = [
        pltpu.make_async_copy(x_ref.at[pl.ds(16 * j, 16)], xb.at[4 * p + j, ax, core], wsem.at[j]) for j in range(4)]
    loads += [
        pltpu.make_async_copy(w1_ref.at[:, lanes(1 - y, half)], w1s, wsem.at[4]),
        pltpu.make_async_copy(w1_ref.at[:, lanes(y, half)], w1o, wsem.at[5]),
        pltpu.make_async_copy(w2_ref, w2, wsem.at[6]),
    ]
    for load in loads:
        load.start()

    barrier = pltpu.get_barrier_semaphore()
    for device in (ypeer, cpeer, xpeer, dpeer, front):
        pl.semaphore_signal(barrier, inc=1, device_id=device, device_id_type=MESH)

    @pl.when(middle)
    def _():
        pl.semaphore_signal(barrier, inc=1, device_id=back, device_id_type=MESH)
        pl.semaphore_wait(barrier, 6)

    @pl.when(edge)
    def _():
        pl.semaphore_wait(barrier, 5)

    def x_front(g):
        pair = xb.at[g, :, core]
        rcopy(pair, pair, xfs, xzr.at[g], front).start()

    def x_back(g):
        pair = xb.at[g, :, core]
        rcopy(pair, pair, xbs, xzr.at[g], back).start()

    def pair_to_core(g):
        pair = xb.at[g, :, core]
        rcopy(pair, pair, xc2s, xc2r.at[g], cpeer).start()

    def own_arrived(j):
        piece = xb.at[4 * p + j, 1 - ax, core]
        arrived(piece, xxr.at[j])
        rcopy(piece, piece, xc1s, xc1r.at[j], cpeer).start()
        x_front(4 * p + j)

        @pl.when(middle & (j < 2))
        def _():
            x_back(4 * p + j)

    for j in range(4):
        piece = xb.at[4 * p + j, ax, core]
        loads[j].wait()
        rcopy(piece, piece, xc0s, xc0r.at[j], cpeer).start()
        rcopy(piece, piece, xxs, xxr.at[j], xpeer).start()
    loads[4].wait()

    def chunk(u):
        place = (u - 2) // 2
        base = jnp.where(edge, pick(place, tuple(enumerate(EDGE))), pick(place, tuple(enumerate(MIDDLE))))
        other = 8 * plane(base // 2) + 4 * lax.rem(base, 2) + 2 * lax.rem(u, 2)
        return jnp.where(u < 4, 8 * p + u, jnp.where(u < 16, other, 8 * p + u - 12))

    def chunk1(u):
        turn = u // 2
        first = 8 * p + 2 * lax.rem(u, 2) + turn + ax - 2 * turn * ax
        return jnp.where(u < 4, first, chunk(u))

    def rows_of(ref, n, count):
        return ref.at[pl.ds(n, count)]

    def product(xv, w, count):
        z = jnp.dot(xv.reshape(count * ROWS, xv.shape[-1]), w[...], preferred_element_type=jnp.float32)
        return z.reshape(count, ROWS, z.shape[1])

    def layer1(n, count, start):
        g, h = n // 2, lax.rem(n, 2)
        if count == 2:
            arrived(xb.at[g, :, 1 - core], xc2r.at[g])
            xv = xb[g]
        else:
            j = lax.rem(g, 4)

            @pl.when(h == ax)
            def _():
                arrived(xb.at[g, h, 1 - core], xc0r.at[j])

            @pl.when(h != ax)
            def _():
                arrived(xb.at[g, h, 1 - core], xc1r.at[j])

            xv = xb[g, h]
        cs[pl.ds(n, count)] = product(xv, w1s, count)
        rcopy(rows_of(cs, n, count), rows_of(cr, n, count), css, crr.at[n], ypeer).start()
        if count == 1:
            @pl.when(start)
            def _():
                loads[5].wait()

        co[pl.ds(n, count)] = product(xv, w1o, count)

    def layer1_last(n, j):
        arrived(xb.at[4 * p + j, ax, 1 - core], xc0r.at[j])
        arrived(xb.at[4 * p + j, 1 - ax, 1 - core], xc1r.at[j])
        xv = xb[4 * p + j]
        cs[pl.ds(n, 2)] = product(xv, w1s, 2)
        for i in range(2):
            rcopy(rows_of(cs, n + i, 1), rows_of(cr, n + i, 1), css, crr.at[n + i], ypeer).start()
        co[pl.ds(n, 2)] = product(xv, w1o, 2)

    def h_piece(n, count, owner, width):
        return hb.at[pl.ds(n, count), :, lanes(owner, width)]

    def activation(n, count):
        arrived(rows_of(cr, n, count), crr.at[n])
        c = (co[pl.ds(n, count)] + cr[pl.ds(n, count)]).astype(jnp.bfloat16).astype(jnp.float32)
        h = jax.nn.gelu(c, approximate=True).astype(jnp.bfloat16)
        hb[pl.ds(n, count), :, lanes(2 * a + y, half)] = h
        piece = h_piece(n, count, 2 * a + y, half)
        rcopy(piece, piece, hys, hyr.at[n], ypeer).start()
        rcopy(piece, piece, hxs, hxr.at[n], xpeer).start()

    def pass_y(n, count):
        piece = h_piece(n, count, 2 * a + 1 - y, half)
        arrived(piece, hyr.at[n])
        rcopy(piece, piece, hxs, hxr.at[n], xpeer).start()
        piece = h_piece(n, count, 2 * a, 2 * half)
        rcopy(piece, piece, hcs, hcr.at[n], cpeer).start()

    def pass_x(n, count):
        piece = h_piece(n, count, 2 * a_x, 2 * half)
        arrived(piece, hxr.at[n])
        rcopy(piece, piece, hcs, hcr.at[n], cpeer).start()

    def layer2(n, own):
        if own is None:
            arrived(h_piece(n, 2, 0, 4 * half), hcr.at[n])
        elif own is True:
            arrived(h_piece(n, 1, 0, 4 * half), hcr.at[n])
            arrived(h_piece(n + 1, 1, 0, 4 * half), hcr.at[n + 1])
        else:
            @pl.when(own)
            def _():
                arrived(h_piece(n, 1, 0, 4 * half), hcr.at[n])
                arrived(h_piece(n + 1, 1, 0, 4 * half), hcr.at[n + 1])

            @pl.when(jnp.logical_not(own))
            def _():
                arrived(h_piece(n, 2, 0, 4 * half), hcr.at[n])

        zp[pl.ds(n, 2)] = product(hb[pl.ds(n, 2)], w2, 2)

    def z_send(n, to, sems, device):
        rcopy(rows_of(zp, n, 2), rows_of(to, n, 2), zss, sems.at[n], device).start()

    def add(n, count, ref):
        zp[pl.ds(n, count)] = zp[pl.ds(n, count)] + ref[pl.ds(n, count)]

    def out_piece(i, c, j, device):
        rcopy(ob.at[i, c], o_ref.at[j, :, lanes(a, half)], oss, orr, device).start()

    def out_own(i, j):
        pltpu.make_async_copy(ob.at[i, core], o_ref.at[j, :, lanes(a, half)], orr).start()
        out_piece(i, 1 - core, j, cpeer)

    def out_other(i, j):
        out_piece(i, core, j, xpeer)
        out_piece(i, 1 - core, j, dpeer)

    def partials_arrived(n):
        arrived(rows_of(zf, n, 2), zfr.at[n])

        @pl.when(middle)
        def _():
            arrived(rows_of(zb, n, 2), zbr.at[n])

    def finish(j):
        n = 8 * p + 2 * j
        partials_arrived(n)
        add(n, 2, zf)

        @pl.when(middle)
        def _():
            add(n, 2, zb)

        ob[pl.ds(2 * j, 2)] = zp[pl.ds(n, 2)].astype(jnp.bfloat16).reshape((2,) + ob.shape[1:])
        out_other(2 * j + 1 - ax, j)
        out_own(2 * j + ax, j)

    def z_edge(n):
        z_send(n, zb, zbr, front)

    def z_middle(n):
        arrived(rows_of(zb, n, 2), zbr.at[n])
        add(n, 2, zb)
        z_send(n, zf, zfr, front)

    def z_back(n):
        arrived(rows_of(zf, n, 2), zfr.at[n])
        add(n, 2, zf)
        z_send(n, zf, zfr, back)

    def step(s, carry):
        def each(u, event):
            @pl.when((u >= 0) & (u < 4))
            def _():
                event(u, 1)

            @pl.when(u >= 4)
            def _():
                event(u, 2)

        each(s, lambda u, count: layer1(chunk1(u), count, s == 0))
        each(s - LF, lambda u, count: pass_y(chunk1(u), count))

        @pl.when(s == 1)
        def _():
            own_arrived(0)

        @pl.when((s >= 1) & (s < 4))
        def _():
            own_arrived(s)

        group = pick(s, [(at, 4 * k + j) for at, k, j in X_EDGE], -1)

        @pl.when(edge & (group >= 0))
        def _():
            g = 4 * plane(group // 4) + lax.rem(group, 4)
            arrived(xb.at[g, :, core], xzr.at[g])
            pair_to_core(g)

        group_b = pick(s, [(at, 4 * k + j) for at, k, j in X_BACK], -1)

        @pl.when(middle & (group_b >= 0))
        def _():
            g = 4 * plane(group_b // 4) + lax.rem(group_b, 4)
            arrived(xb.at[g, :, core], xzr.at[g])
            x_front(g)
            pair_to_core(g)

        group_f = pick(s, [(at, 4 * k + j) for at, k, j in X_FRONT], -1)

        @pl.when(middle & (group_f >= 0))
        def _():
            g = 4 * plane(group_f // 4) + lax.rem(group_f, 4)
            arrived(xb.at[g, :, core], xzr.at[g])
            x_back(g)
            pair_to_core(g)

        late = pick(s, [(at, j) for at, _, j in X_LATE], -1)

        @pl.when(middle & (late >= 0))
        def _():
            x_back(4 * p + late)

        each(s - LC, lambda u, count: pass_x(chunk(u), count))

        t = s - L2

        @pl.when(t == 1)
        def _():
            loads[6].wait()

        @pl.when((t == 1) | (t >= 3))
        def _():
            layer2(chunk(jnp.where(t < 4, t - 1, t)), t < 4)

        @pl.when(edge & (t >= 4))
        def _():
            z_edge(chunk(t))

        @pl.when(middle & (t >= 8))
        def _():
            z_middle(chunk(t))

        each(s - LH, lambda u, count: activation(chunk1(u), count))
        return carry

    lax.fori_loop(0, LOOPED, step, 0)

    def tail(kind, u):
        n, count = chunk(jnp.int32(u)), 2 if u < 16 else 1
        if kind == "M":
            layer1_last(n, 2 + (u - 16) // 2)
        elif kind == "H":
            activation(n, count)
        elif kind == "F":
            pass_y(n, count)
        elif kind == "C":
            pass_x(n, count)
        elif kind == "L":
            layer2(n, None if u < 16 else True)
        elif kind == "Z":
            pl.when(edge)(lambda: z_edge(n))
            pl.when(middle)(lambda: z_middle(n))
        elif kind == "B":
            pl.when(middle)(lambda: z_back(8 * plane(0) + 2 * u))
        elif kind == "O":
            finish(u)

    for event in TAIL.split():
        tail(event[0], int(event[1:]))

    arrived(o_ref, orr)
    sent(ob.at[pl.ds(0, 6)], oss)
    sent(cs, css)
    for sem, width in ((hys, half), (hxs, 2 * half), (hcs, 4 * half)):
        sent(hb.at[:, :, pl.ds(0, width)], sem)
    sent(zp.at[pl.ds(0, 24)], zss)
    for sem in (xxs, xc0s, xc1s):
        sent(xb.at[pl.ds(0, 4), 0, 0], sem)
    sent(xb.at[pl.ds(0, 12), :, 0], xc2s)

    @pl.when(edge)
    def _():
        sent(xb.at[pl.ds(0, 4), :, 0], xfs)

    @pl.when(middle)
    def _():
        sent(xb.at[pl.ds(0, 8), :, 0], xfs)
        sent(xb.at[pl.ds(0, 12), :, 0], xbs)


def solution(mesh):
    def body(x, w1, w2):
        r, d = x.shape
        k1, n1 = w1.shape
        k2, n2 = w2.shape
        half = n1 // 2
        f32, bf16 = jnp.float32, jnp.bfloat16
        dma = pltpu.SemaphoreType.DMA
        one, four, groups, chunks = dma(()), dma((4,)), dma((16,)), dma((CHUNKS,))
        out = pl.pallas_call(
            kernel,
            out_shape=jax.ShapeDtypeStruct((4, r // 4, d), bf16),
            in_specs=[pl.BlockSpec(memory_space=pltpu.HBM)] * 3,
            out_specs=pl.BlockSpec(memory_space=pl.ANY),
            scratch_shapes=[
                pltpu.VMEM((k1, half), bf16),
                pltpu.VMEM((k1, half), bf16),
                pltpu.VMEM((k2, n2), bf16),
                pltpu.VMEM((16, 2, 2, 16, d), bf16),
                pltpu.VMEM((CHUNKS, ROWS, half), f32),
                pltpu.VMEM((CHUNKS, ROWS, half), f32),
                pltpu.VMEM((CHUNKS, ROWS, half), f32),
                pltpu.VMEM((CHUNKS, ROWS, k2), bf16),
                pltpu.VMEM((CHUNKS, ROWS, n2), f32),
                pltpu.VMEM((CHUNKS, ROWS, n2), f32),
                pltpu.VMEM((CHUNKS, ROWS, n2), f32),
                pltpu.VMEM((8, 2, 16, n2), bf16),
                dma((7,)),
                one, four,
                one, one, groups,
                one, four, one, four, one, groups,
                one, chunks,
                one, chunks,
                one, chunks,
                one, chunks,
                one, chunks, chunks,
                one, one,
            ],
            compiler_params=pltpu.CompilerParams(
                collective_id=0, has_side_effects=True, vmem_limit_bytes=48 * 1024 * 1024),
            name="mlp",
        )(x, w1, w2)
        return out.reshape(r, d)

    return jax.shard_map(
        body,
        mesh=mesh,
        in_specs=(P(("cx", "cz"), "cy"), P("cy", ("cz", "cx")), P("cz", ("cy", "cx"))),
        out_specs=P(("cx", "cz"), "cy"),
        check_vma=False,
    )
```

```python
import jax
import jax.numpy as jnp
from jax import lax
from jax.experimental import pallas as pl
from jax.experimental.pallas import tpu as pltpu
from jax.sharding import PartitionSpec as P

MESH = pl.DeviceIdType.MESH
CHUNKS, ROWS = 32, 32
LOOPED = 16
LH, LF, LC, L2 = 1, 3, 5, 6
TAIL = (
    ("L", 10), ("F", 13), ("Z", 10), ("C", 11), ("M", 16), ("L", 11), ("H", 15), ("C", 12), ("Z", 11), ("C", 13),
    ("M", 18), ("F", 14), ("L", 12), ("H", 16), ("B", 0), ("Z", 12), ("L", 13), ("H", 17), ("C", 14), ("B", 1),
    ("F", 15), ("Z", 13), ("L", 14), ("H", 18), ("Z", 14), ("B", 2), ("H", 19), ("F", 16), ("C", 15), ("F", 17),
    ("F", 18), ("L", 15), ("Z", 15), ("B", 3), ("F", 19), ("O", 0), ("C", 16), ("C", 17), ("O", 1), ("C", 18),
    ("L", 16), ("C", 19), ("O", 2), ("L", 18), ("O", 3),
)
EDGE = (0, 2, 4, 6, 7, 5, 3, 1)
MIDDLE = (2, 0, 1, 4, 6, 7, 5, 3)
X_EDGE = tuple((3 + e, k, j) for e, (k, j) in enumerate(
    ((1, 0), (1, 1), (2, 0), (2, 1), (3, 0), (3, 1), (3, 2), (3, 3), (2, 2), (2, 3), (1, 2), (1, 3))))
X_BACK = tuple((3 + j, 0, j) for j in range(4))
X_FRONT = tuple((3 + e, k, j) for e, (k, j) in enumerate(
    ((2, 0), (2, 1), (3, 0), (3, 1), (3, 2), (3, 3), (2, 2), (2, 3))))
X_LATE_FRONT = ((7, 2), (8, 3))
X_LATE_BACK = ((10, 2), (11, 3))


def pick(index, pairs, default=0):
    value = jnp.int32(default)
    for key, item in pairs:
        value = jnp.where(index == key, jnp.int32(item), value)
    return value


def kernel(x_ref, w1_ref, w2_ref, o_ref, w1s, w1o, w2, xb, cs, co, cr, hb, zp, zf, zb, ob,
           wsem, xxs, xxr, xfs, xbs, xzr, xc0s, xc0r, xc1s, xc1r, xc2s, xc2r, css, crr, hys, hyr, hxs, hxr,
           hcs, hcr, zss, zfr, zbr, oss, orr):
    p, y, a = lax.axis_index("cz"), lax.axis_index("cy"), lax.axis_index("cx")
    core, ax = lax.rem(a, 2), a // 2
    half = w1s.shape[1]
    a_c, a_x = a + 1 - 2 * core, lax.rem(a + 2, 4)
    a_d = lax.rem(a_c + 2, 4)
    low = p < 2
    edge = (p == 0) | (p == 3)
    middle = (p > 0) & (p < 3)
    ypeer, cpeer, xpeer, dpeer = {"cy": 1 - y}, {"cx": a_c}, {"cx": a_x}, {"cx": a_d}
    front = {"cz": jnp.where(low, p + 1, p - 1)}
    back = {"cz": jnp.where(edge, p, jnp.where(low, p - 1, p + 1))}

    def rcopy(src, dst, ss, rs, device):
        return pltpu.make_async_remote_copy(
            src_ref=src, dst_ref=dst, send_sem=ss, recv_sem=rs, device_id=device, device_id_type=MESH)

    def arrived(ref, sem):
        rcopy(ref, ref, oss, sem, cpeer).wait_recv()

    def sent(ref, sem):
        rcopy(ref, ref, sem, orr, cpeer).wait_send()

    def lanes(owner, width):
        return pl.ds(pl.multiple_of(owner * half, 128), width)

    def plane(k):
        return jnp.where(low, k, 3 - k)

    loads = [
        pltpu.make_async_copy(x_ref.at[pl.ds(16 * j, 16)], xb.at[4 * p + j, ax, core], wsem.at[j]) for j in range(4)]
    loads += [
        pltpu.make_async_copy(w1_ref.at[:, lanes(1 - y, half)], w1s, wsem.at[4]),
        pltpu.make_async_copy(w1_ref.at[:, lanes(y, half)], w1o, wsem.at[5]),
        pltpu.make_async_copy(w2_ref, w2, wsem.at[6]),
    ]
    for load in loads:
        load.start()

    barrier = pltpu.get_barrier_semaphore()
    for device in (ypeer, cpeer, xpeer, dpeer, front):
        pl.semaphore_signal(barrier, inc=1, device_id=device, device_id_type=MESH)

    @pl.when(middle)
    def _():
        pl.semaphore_signal(barrier, inc=1, device_id=back, device_id_type=MESH)
        pl.semaphore_wait(barrier, 6)

    @pl.when(edge)
    def _():
        pl.semaphore_wait(barrier, 5)

    def x_front(g):
        pair = xb.at[g, :, core]
        rcopy(pair, pair, xfs, xzr.at[g], front).start()

    def x_back(g):
        pair = xb.at[g, :, core]
        rcopy(pair, pair, xbs, xzr.at[g], back).start()

    def pair_to_core(g):
        pair = xb.at[g, :, core]
        rcopy(pair, pair, xc2s, xc2r.at[g], cpeer).start()

    def own_arrived(j):
        piece = xb.at[4 * p + j, 1 - ax, core]
        arrived(piece, xxr.at[j])
        rcopy(piece, piece, xc1s, xc1r.at[j], cpeer).start()

        @pl.when(edge | (j < 2))
        def _():
            x_front(4 * p + j)

        @pl.when(middle & (j < 2))
        def _():
            x_back(4 * p + j)

    for j in range(4):
        piece = xb.at[4 * p + j, ax, core]
        loads[j].wait()
        rcopy(piece, piece, xc0s, xc0r.at[j], cpeer).start()
        rcopy(piece, piece, xxs, xxr.at[j], xpeer).start()
    loads[4].wait()

    def chunk(u):
        place = (u - 2) // 2
        base = jnp.where(edge, pick(place, tuple(enumerate(EDGE))), pick(place, tuple(enumerate(MIDDLE))))
        other = 8 * plane(base // 2) + 4 * lax.rem(base, 2) + 2 * lax.rem(u, 2)
        return jnp.where(u < 4, 8 * p + u, jnp.where(u < 16, other, 8 * p + u - 12))

    def chunk1(u):
        turn = u // 2
        first = 8 * p + 2 * lax.rem(u, 2) + turn + ax - 2 * turn * ax
        return jnp.where(u < 4, first, chunk(u))

    def rows_of(ref, n, count):
        return ref.at[pl.ds(n, count)]

    def product(xv, w, count):
        z = jnp.dot(xv.reshape(count * ROWS, xv.shape[-1]), w[...], preferred_element_type=jnp.float32)
        return z.reshape(count, ROWS, z.shape[1])

    def layer1(n, count, start):
        g, h = n // 2, lax.rem(n, 2)
        if count == 2:
            arrived(xb.at[g, :, 1 - core], xc2r.at[g])
            xv = xb[g]
        else:
            j = lax.rem(g, 4)

            @pl.when(h == ax)
            def _():
                arrived(xb.at[g, h, 1 - core], xc0r.at[j])

            @pl.when(h != ax)
            def _():
                arrived(xb.at[g, h, 1 - core], xc1r.at[j])

            xv = xb[g, h]
        cs[pl.ds(n, count)] = product(xv, w1s, count)
        rcopy(rows_of(cs, n, count), rows_of(cr, n, count), css, crr.at[n], ypeer).start()
        if count == 1:
            @pl.when(start)
            def _():
                loads[5].wait()

        co[pl.ds(n, count)] = product(xv, w1o, count)

    def layer1_last(n, j):
        arrived(xb.at[4 * p + j, ax, 1 - core], xc0r.at[j])
        arrived(xb.at[4 * p + j, 1 - ax, 1 - core], xc1r.at[j])
        xv = xb[4 * p + j]
        cs[pl.ds(n, 2)] = product(xv, w1s, 2)
        for i in range(2):
            rcopy(rows_of(cs, n + i, 1), rows_of(cr, n + i, 1), css, crr.at[n + i], ypeer).start()
        co[pl.ds(n, 2)] = product(xv, w1o, 2)

    def h_piece(n, count, owner, width):
        return hb.at[pl.ds(n, count), :, lanes(owner, width)]

    def activation(n, count):
        arrived(rows_of(cr, n, count), crr.at[n])
        c = (co[pl.ds(n, count)] + cr[pl.ds(n, count)]).astype(jnp.bfloat16).astype(jnp.float32)
        h = jax.nn.gelu(c, approximate=True).astype(jnp.bfloat16)
        hb[pl.ds(n, count), :, lanes(2 * a + y, half)] = h
        piece = h_piece(n, count, 2 * a + y, half)
        rcopy(piece, piece, hys, hyr.at[n], ypeer).start()
        rcopy(piece, piece, hxs, hxr.at[n], xpeer).start()

    def pass_y(n, count):
        piece = h_piece(n, count, 2 * a + 1 - y, half)
        arrived(piece, hyr.at[n])
        rcopy(piece, piece, hxs, hxr.at[n], xpeer).start()
        piece = h_piece(n, count, 2 * a, 2 * half)
        rcopy(piece, piece, hcs, hcr.at[n], cpeer).start()

    def pass_x(n, count):
        piece = h_piece(n, count, 2 * a_x, 2 * half)
        arrived(piece, hxr.at[n])
        rcopy(piece, piece, hcs, hcr.at[n], cpeer).start()

    def layer2(n, own):
        if own is None:
            arrived(h_piece(n, 2, 0, 4 * half), hcr.at[n])
        elif own is True:
            arrived(h_piece(n, 1, 0, 4 * half), hcr.at[n])
            arrived(h_piece(n + 1, 1, 0, 4 * half), hcr.at[n + 1])
        else:
            @pl.when(own)
            def _():
                arrived(h_piece(n, 1, 0, 4 * half), hcr.at[n])
                arrived(h_piece(n + 1, 1, 0, 4 * half), hcr.at[n + 1])

            @pl.when(jnp.logical_not(own))
            def _():
                arrived(h_piece(n, 2, 0, 4 * half), hcr.at[n])

        zp[pl.ds(n, 2)] = product(hb[pl.ds(n, 2)], w2, 2)

    def z_send(n, to, sems, device):
        rcopy(rows_of(zp, n, 2), rows_of(to, n, 2), zss, sems.at[n], device).start()

    def add(n, count, ref):
        zp[pl.ds(n, count)] = zp[pl.ds(n, count)] + ref[pl.ds(n, count)]

    def out_piece(i, c, j, device):
        rcopy(ob.at[i, c], o_ref.at[j, :, lanes(a, half)], oss, orr, device).start()

    def out_own(i, j):
        pltpu.make_async_copy(ob.at[i, core], o_ref.at[j, :, lanes(a, half)], orr).start()
        out_piece(i, 1 - core, j, cpeer)

    def out_other(i, j):
        out_piece(i, core, j, xpeer)
        out_piece(i, 1 - core, j, dpeer)

    def partials_arrived(n):
        arrived(rows_of(zf, n, 2), zfr.at[n])

        @pl.when(middle)
        def _():
            arrived(rows_of(zb, n, 2), zbr.at[n])

    def finish(j):
        n = 8 * p + 2 * j
        partials_arrived(n)
        add(n, 2, zf)

        @pl.when(middle)
        def _():
            add(n, 2, zb)

        ob[pl.ds(2 * j, 2)] = zp[pl.ds(n, 2)].astype(jnp.bfloat16).reshape((2,) + ob.shape[1:])
        out_other(2 * j + 1 - ax, j)
        out_own(2 * j + ax, j)

    def z_edge(n):
        z_send(n, zb, zbr, front)

    def z_middle(n):
        arrived(rows_of(zb, n, 2), zbr.at[n])
        add(n, 2, zb)
        z_send(n, zf, zfr, front)

    def z_back(n):
        arrived(rows_of(zf, n, 2), zfr.at[n])
        add(n, 2, zf)
        z_send(n, zf, zfr, back)

    def step(s, carry):
        def each(u, event):
            @pl.when((u >= 0) & (u < 4))
            def _():
                event(u, 1)

            @pl.when(u >= 4)
            def _():
                event(u, 2)

        each(s, lambda u, count: layer1(chunk1(u), count, s == 0))
        each(s - LF, lambda u, count: pass_y(chunk1(u), count))

        @pl.when((s >= 1) & (s < 5))
        def _():
            own_arrived(s - 1)

        group = pick(s, [(at, 4 * k + j) for at, k, j in X_EDGE], -1)

        @pl.when(edge & (group >= 0))
        def _():
            g = 4 * plane(group // 4) + lax.rem(group, 4)
            arrived(xb.at[g, :, core], xzr.at[g])
            pair_to_core(g)

        group_b = pick(s, [(at, 4 * k + j) for at, k, j in X_BACK], -1)

        @pl.when(middle & (group_b >= 0))
        def _():
            g = 4 * plane(group_b // 4) + lax.rem(group_b, 4)
            arrived(xb.at[g, :, core], xzr.at[g])
            x_front(g)
            pair_to_core(g)

        group_f = pick(s, [(at, 4 * k + j) for at, k, j in X_FRONT], -1)

        @pl.when(middle & (group_f >= 0))
        def _():
            g = 4 * plane(group_f // 4) + lax.rem(group_f, 4)
            arrived(xb.at[g, :, core], xzr.at[g])
            x_back(g)
            pair_to_core(g)

        for order, send in ((X_LATE_FRONT, x_front), (X_LATE_BACK, x_back)):
            late = pick(s, order, -1)

            @pl.when(middle & (late >= 0))
            def _():
                send(4 * p + late)

        each(s - LC, lambda u, count: pass_x(chunk(u), count))

        t = s - L2

        @pl.when(t == 1)
        def _():
            loads[6].wait()

        @pl.when((t == 1) | (t >= 3))
        def _():
            layer2(chunk(jnp.where(t < 4, t - 1, t)), t < 4)

        @pl.when(edge & (t >= 4))
        def _():
            z_edge(chunk(t))

        @pl.when(middle & (t >= 8))
        def _():
            z_middle(chunk(t))

        each(s - LH, lambda u, count: activation(chunk1(u), count))
        return carry

    lax.fori_loop(0, LOOPED, step, 0)

    def tail(kind, u):
        n, count = chunk(jnp.int32(u)), 2 if u < 16 else 1
        if kind == "M":
            layer1_last(n, 2 + (u - 16) // 2)
        elif kind == "H":
            activation(n, count)
        elif kind == "F":
            pass_y(n, count)
        elif kind == "C":
            pass_x(n, count)
        elif kind == "L":
            layer2(n, None if u < 16 else True)
        elif kind == "Z":
            pl.when(edge)(lambda: z_edge(n))
            pl.when(middle)(lambda: z_middle(n))
        elif kind == "B":
            pl.when(middle)(lambda: z_back(8 * plane(0) + 2 * u))
        elif kind == "O":
            finish(u)

    for kind, u in TAIL:
        tail(kind, u)

    arrived(o_ref, orr)
    sent(ob.at[pl.ds(0, 6)], oss)
    sent(cs, css)
    for sem, width in ((hys, half), (hxs, 2 * half), (hcs, 4 * half)):
        sent(hb.at[:, :, pl.ds(0, width)], sem)
    sent(zp.at[pl.ds(0, 24)], zss)
    for sem in (xxs, xc0s, xc1s):
        sent(xb.at[pl.ds(0, 4), 0, 0], sem)
    sent(xb.at[pl.ds(0, 12), :, 0], xc2s)

    @pl.when(edge)
    def _():
        sent(xb.at[pl.ds(0, 4), :, 0], xfs)

    @pl.when(middle)
    def _():
        sent(xb.at[pl.ds(0, 8), :, 0], xfs)
        sent(xb.at[pl.ds(0, 12), :, 0], xbs)


def solution(mesh):
    def body(x, w1, w2):
        r, d = x.shape
        k1, n1 = w1.shape
        k2, n2 = w2.shape
        half = n1 // 2
        f32, bf16 = jnp.float32, jnp.bfloat16
        dma = pltpu.SemaphoreType.DMA
        one, four, groups, chunks = dma(()), dma((4,)), dma((16,)), dma((CHUNKS,))
        out = pl.pallas_call(
            kernel,
            out_shape=jax.ShapeDtypeStruct((4, r // 4, d), bf16),
            in_specs=[pl.BlockSpec(memory_space=pltpu.HBM)] * 3,
            out_specs=pl.BlockSpec(memory_space=pl.ANY),
            scratch_shapes=[
                pltpu.VMEM((k1, half), bf16),
                pltpu.VMEM((k1, half), bf16),
                pltpu.VMEM((k2, n2), bf16),
                pltpu.VMEM((16, 2, 2, 16, d), bf16),
                pltpu.VMEM((CHUNKS, ROWS, half), f32),
                pltpu.VMEM((CHUNKS, ROWS, half), f32),
                pltpu.VMEM((CHUNKS, ROWS, half), f32),
                pltpu.VMEM((CHUNKS, ROWS, k2), bf16),
                pltpu.VMEM((CHUNKS, ROWS, n2), f32),
                pltpu.VMEM((CHUNKS, ROWS, n2), f32),
                pltpu.VMEM((CHUNKS, ROWS, n2), f32),
                pltpu.VMEM((8, 2, 16, n2), bf16),
                dma((7,)),
                one, four,
                one, one, groups,
                one, four, one, four, one, groups,
                one, chunks,
                one, chunks,
                one, chunks,
                one, chunks,
                one, chunks, chunks,
                one, one,
            ],
            compiler_params=pltpu.CompilerParams(
                collective_id=0, has_side_effects=True, vmem_limit_bytes=48 * 1024 * 1024),
            name="mlp",
        )(pltpu.with_memory_space_constraint(x, pltpu.HBM), w1, w2)
        return out.reshape(r, d)

    return jax.shard_map(
        body,
        mesh=mesh,
        in_specs=(P(("cx", "cz"), "cy"), P("cy", ("cz", "cx")), P("cz", ("cy", "cx"))),
        out_specs=P(("cx", "cz"), "cy"),
        check_vma=False,
    )
```

```python
import jax
import jax.numpy as jnp
from jax import lax
from jax.experimental import pallas as pl
from jax.experimental.pallas import tpu as pltpu
from jax.sharding import PartitionSpec as P

MESH = pl.DeviceIdType.MESH
CHUNKS, ROWS = 32, 32
LOOPED = 16
LH, LF, LC, L2 = 1, 3, 5, 6
TAIL = (
    ("L", 10), ("F", 13), ("Z", 10), ("C", 11), ("M", 16), ("L", 11), ("H", 15), ("C", 12), ("Z", 11), ("C", 13),
    ("M", 18), ("F", 14), ("L", 12), ("H", 16), ("B", 0), ("Z", 12), ("L", 13), ("H", 17), ("C", 14), ("B", 1),
    ("F", 15), ("Z", 13), ("L", 14), ("H", 18), ("Z", 14), ("B", 2), ("H", 19), ("F", 16), ("C", 15), ("F", 17),
    ("F", 18), ("L", 15), ("Z", 15), ("B", 3), ("F", 19), ("O", 0), ("C", 16), ("C", 17), ("O", 1), ("C", 18),
    ("L", 16), ("C", 19), ("O", 2), ("L", 18), ("O", 3),
)
EDGE = (0, 2, 4, 6, 7, 5, 3, 1)
MIDDLE = (2, 0, 1, 4, 6, 7, 5, 3)
X_EDGE = tuple((3 + e, k, j) for e, (k, j) in enumerate(
    ((1, 0), (1, 1), (2, 0), (2, 1), (3, 0), (3, 1), (3, 2), (3, 3), (2, 2), (2, 3), (1, 2), (1, 3))))
X_BACK = tuple((3 + j, 0, j) for j in range(4))
X_FRONT = tuple((3 + e, k, j) for e, (k, j) in enumerate(
    ((2, 0), (2, 1), (3, 0), (3, 1), (3, 2), (3, 3), (2, 2), (2, 3))))
X_LATE_FRONT = ((7, 2), (8, 3))
X_LATE_BACK = ((10, 2), (11, 3))


def pick(index, pairs, default=0):
    value = jnp.int32(default)
    for key, item in pairs:
        value = jnp.where(index == key, jnp.int32(item), value)
    return value


def kernel(x_ref, w1_ref, w2_ref, o_ref, w1s, w1o, w2, xb, cs, co, cr, hb, zp, zf, zb, ob,
           wsem, xxs, xxr, xfs, xbs, xzr, xc0s, xc0r, xc1s, xc1r, xc2s, xc2r, css, crr, hys, hyr, hxs, hxr,
           hcs, hcr, zss, zfr, zbr, oss, orr):
    p, y, a = lax.axis_index("cz"), lax.axis_index("cy"), lax.axis_index("cx")
    core, ax = lax.rem(a, 2), a // 2
    half = w1s.shape[1]
    a_c, a_x = a + 1 - 2 * core, lax.rem(a + 2, 4)
    a_d = lax.rem(a_c + 2, 4)
    low = p < 2
    edge = (p == 0) | (p == 3)
    middle = (p > 0) & (p < 3)
    ypeer, cpeer, xpeer, dpeer = {"cy": 1 - y}, {"cx": a_c}, {"cx": a_x}, {"cx": a_d}
    front = {"cz": jnp.where(low, p + 1, p - 1)}
    back = {"cz": jnp.where(edge, p, jnp.where(low, p - 1, p + 1))}

    def rcopy(src, dst, ss, rs, device):
        return pltpu.make_async_remote_copy(
            src_ref=src, dst_ref=dst, send_sem=ss, recv_sem=rs, device_id=device, device_id_type=MESH)

    def arrived(ref, sem):
        rcopy(ref, ref, oss, sem, cpeer).wait_recv()

    def sent(ref, sem):
        rcopy(ref, ref, sem, orr, cpeer).wait_send()

    def lanes(owner, width):
        return pl.ds(pl.multiple_of(owner * half, 128), width)

    def plane(k):
        return jnp.where(low, k, 3 - k)

    loads = [
        pltpu.make_async_copy(x_ref.at[pl.ds(16 * j, 16)], xb.at[4 * p + j, ax, core], wsem.at[j]) for j in range(4)]
    loads += [
        pltpu.make_async_copy(w1_ref.at[:, lanes(1 - y, half)], w1s, wsem.at[4]),
        pltpu.make_async_copy(w1_ref.at[:, lanes(y, half)], w1o, wsem.at[5]),
        pltpu.make_async_copy(w2_ref, w2, wsem.at[6]),
    ]
    for load in loads[:6]:
        load.start()

    barrier = pltpu.get_barrier_semaphore()
    for device in (ypeer, cpeer, xpeer, dpeer, front):
        pl.semaphore_signal(barrier, inc=1, device_id=device, device_id_type=MESH)

    @pl.when(middle)
    def _():
        pl.semaphore_signal(barrier, inc=1, device_id=back, device_id_type=MESH)
        pl.semaphore_wait(barrier, 6)

    @pl.when(edge)
    def _():
        pl.semaphore_wait(barrier, 5)

    def x_front(g):
        pair = xb.at[g, :, core]
        rcopy(pair, pair, xfs, xzr.at[g], front).start()

    def x_back(g):
        pair = xb.at[g, :, core]
        rcopy(pair, pair, xbs, xzr.at[g], back).start()

    def x_part(j, owner):
        part = xb.at[4 * p + j, owner, core]
        rcopy(part, part, xfs, xzr.at[4 * p + j], front).start()

        @pl.when(middle)
        def _():
            rcopy(part, part, xbs, xzr.at[4 * p + j], back).start()

    def pair_to_core(g):
        pair = xb.at[g, :, core]
        rcopy(pair, pair, xc2s, xc2r.at[g], cpeer).start()

    def own_arrived(j):
        piece = xb.at[4 * p + j, 1 - ax, core]
        arrived(piece, xxr.at[j])
        rcopy(piece, piece, xc1s, xc1r.at[j], cpeer).start()

        @pl.when(j < 2)
        def _():
            x_part(j, 1 - ax)

        @pl.when(edge & (j >= 2))
        def _():
            x_front(4 * p + j)

    for j in range(4):
        piece = xb.at[4 * p + j, ax, core]
        loads[j].wait()
        rcopy(piece, piece, xc0s, xc0r.at[j], cpeer).start()
        rcopy(piece, piece, xxs, xxr.at[j], xpeer).start()
        if j < 2:
            x_part(j, ax)

    loads[4].wait()
    loads[6].start()

    def chunk(u):
        place = (u - 2) // 2
        base = jnp.where(edge, pick(place, tuple(enumerate(EDGE))), pick(place, tuple(enumerate(MIDDLE))))
        other = 8 * plane(base // 2) + 4 * lax.rem(base, 2) + 2 * lax.rem(u, 2)
        return jnp.where(u < 4, 8 * p + u, jnp.where(u < 16, other, 8 * p + u - 12))

    def chunk1(u):
        turn = u // 2
        first = 8 * p + 2 * lax.rem(u, 2) + turn + ax - 2 * turn * ax
        return jnp.where(u < 4, first, chunk(u))

    def rows_of(ref, n, count):
        return ref.at[pl.ds(n, count)]

    def product(xv, w, count):
        z = jnp.dot(xv.reshape(count * ROWS, xv.shape[-1]), w[...], preferred_element_type=jnp.float32)
        return z.reshape(count, ROWS, z.shape[1])

    def layer1(n, count, start):
        g, h = n // 2, lax.rem(n, 2)
        if count == 2:
            arrived(xb.at[g, :, 1 - core], xc2r.at[g])
            xv = xb[g]
            cs[pl.ds(n, count)] = product(xv, w1s, count)
            rcopy(rows_of(cs, n, count), rows_of(cr, n, count), css, crr.at[n], ypeer).start()
        else:
            j = lax.rem(g, 4)

            def part(c):
                rows = pl.ds(pl.multiple_of(16 * c, 16), 16)
                cs[n, rows] = jnp.dot(xb[g, h, c], w1s[...], preferred_element_type=jnp.float32)
                rcopy(cs.at[n, rows], cr.at[n, rows], css, crr.at[n], ypeer).start()

            part(core)

            @pl.when(h == ax)
            def _():
                arrived(xb.at[g, h, 1 - core], xc0r.at[j])

            @pl.when(h != ax)
            def _():
                arrived(xb.at[g, h, 1 - core], xc1r.at[j])

            part(1 - core)
            xv = xb[g, h]

            @pl.when(start)
            def _():
                loads[5].wait()

        co[pl.ds(n, count)] = product(xv, w1o, count)

    def layer1_last(n, j):
        arrived(xb.at[4 * p + j, ax, 1 - core], xc0r.at[j])
        arrived(xb.at[4 * p + j, 1 - ax, 1 - core], xc1r.at[j])
        xv = xb[4 * p + j]
        cs[pl.ds(n, 2)] = product(xv, w1s, 2)
        for i in range(2):
            rcopy(rows_of(cs, n + i, 1), rows_of(cr, n + i, 1), css, crr.at[n + i], ypeer).start()
        co[pl.ds(n, 2)] = product(xv, w1o, 2)

    def h_piece(n, count, owner, width):
        return hb.at[pl.ds(n, count), :, lanes(owner, width)]

    def activation(n, count):
        arrived(rows_of(cr, n, count), crr.at[n])
        c = (co[pl.ds(n, count)] + cr[pl.ds(n, count)]).astype(jnp.bfloat16).astype(jnp.float32)
        h = jax.nn.gelu(c, approximate=True).astype(jnp.bfloat16)
        hb[pl.ds(n, count), :, lanes(2 * a + y, half)] = h
        piece = h_piece(n, count, 2 * a + y, half)
        rcopy(piece, piece, hys, hyr.at[n], ypeer).start()
        rcopy(piece, piece, hxs, hxr.at[n], xpeer).start()

    def pass_y(n, count):
        piece = h_piece(n, count, 2 * a + 1 - y, half)
        arrived(piece, hyr.at[n])
        rcopy(piece, piece, hxs, hxr.at[n], xpeer).start()
        piece = h_piece(n, count, 2 * a, 2 * half)
        rcopy(piece, piece, hcs, hcr.at[n], cpeer).start()

    def pass_x(n, count):
        piece = h_piece(n, count, 2 * a_x, 2 * half)
        arrived(piece, hxr.at[n])
        rcopy(piece, piece, hcs, hcr.at[n], cpeer).start()

    def layer2(n, own):
        if own is None:
            arrived(h_piece(n, 2, 0, 4 * half), hcr.at[n])
        elif own is True:
            arrived(h_piece(n, 1, 0, 4 * half), hcr.at[n])
            arrived(h_piece(n + 1, 1, 0, 4 * half), hcr.at[n + 1])
        else:
            @pl.when(own)
            def _():
                arrived(h_piece(n, 1, 0, 4 * half), hcr.at[n])
                arrived(h_piece(n + 1, 1, 0, 4 * half), hcr.at[n + 1])

            @pl.when(jnp.logical_not(own))
            def _():
                arrived(h_piece(n, 2, 0, 4 * half), hcr.at[n])

        zp[pl.ds(n, 2)] = product(hb[pl.ds(n, 2)], w2, 2)

    def z_send(n, to, sems, device):
        rcopy(rows_of(zp, n, 2), rows_of(to, n, 2), zss, sems.at[n], device).start()

    def add(n, count, ref):
        zp[pl.ds(n, count)] = zp[pl.ds(n, count)] + ref[pl.ds(n, count)]

    def out_piece(i, c, j, device):
        rcopy(ob.at[i, c], o_ref.at[j, :, lanes(a, half)], oss, orr, device).start()

    def out_own(i, j):
        pltpu.make_async_copy(ob.at[i, core], o_ref.at[j, :, lanes(a, half)], orr).start()
        out_piece(i, 1 - core, j, cpeer)

    def out_other(i, j):
        out_piece(i, core, j, xpeer)
        out_piece(i, 1 - core, j, dpeer)

    def partials_arrived(n):
        arrived(rows_of(zf, n, 2), zfr.at[n])

        @pl.when(middle)
        def _():
            arrived(rows_of(zb, n, 2), zbr.at[n])

    def finish(j):
        n = 8 * p + 2 * j
        partials_arrived(n)
        add(n, 2, zf)

        @pl.when(middle)
        def _():
            add(n, 2, zb)

        ob[pl.ds(2 * j, 2)] = zp[pl.ds(n, 2)].astype(jnp.bfloat16).reshape((2,) + ob.shape[1:])
        out_other(2 * j + 1 - ax, j)
        out_own(2 * j + ax, j)

    def z_edge(n):
        z_send(n, zb, zbr, front)

    def z_middle(n):
        arrived(rows_of(zb, n, 2), zbr.at[n])
        add(n, 2, zb)
        z_send(n, zf, zfr, front)

    def z_back(n):
        arrived(rows_of(zf, n, 2), zfr.at[n])
        add(n, 2, zf)
        z_send(n, zf, zfr, back)

    def step(s, carry):
        def each(u, event):
            @pl.when((u >= 0) & (u < 4))
            def _():
                event(u, 1)

            @pl.when(u >= 4)
            def _():
                event(u, 2)

        each(s, lambda u, count: layer1(chunk1(u), count, s == 0))
        each(s - LF, lambda u, count: pass_y(chunk1(u), count))

        @pl.when((s >= 1) & (s < 5))
        def _():
            own_arrived(s - 1)

        group = pick(s, [(at, 4 * k + j) for at, k, j in X_EDGE], -1)

        @pl.when(edge & (group >= 0))
        def _():
            g = 4 * plane(group // 4) + lax.rem(group, 4)
            arrived(xb.at[g, :, core], xzr.at[g])
            pair_to_core(g)

        group_b = pick(s, [(at, 4 * k + j) for at, k, j in X_BACK], -1)

        @pl.when(middle & (group_b >= 0))
        def _():
            g = 4 * plane(group_b // 4) + lax.rem(group_b, 4)
            arrived(xb.at[g, :, core], xzr.at[g])
            x_front(g)
            pair_to_core(g)

        group_f = pick(s, [(at, 4 * k + j) for at, k, j in X_FRONT], -1)

        @pl.when(middle & (group_f >= 0))
        def _():
            g = 4 * plane(group_f // 4) + lax.rem(group_f, 4)
            arrived(xb.at[g, :, core], xzr.at[g])
            x_back(g)
            pair_to_core(g)

        for order, send in ((X_LATE_FRONT, x_front), (X_LATE_BACK, x_back)):
            late = pick(s, order, -1)

            @pl.when(middle & (late >= 0))
            def _():
                send(4 * p + late)

        each(s - LC, lambda u, count: pass_x(chunk(u), count))

        t = s - L2

        @pl.when(t == 1)
        def _():
            loads[6].wait()

        @pl.when((t == 1) | (t >= 3))
        def _():
            layer2(chunk(jnp.where(t < 4, t - 1, t)), t < 4)

        @pl.when(edge & (t >= 4))
        def _():
            z_edge(chunk(t))

        @pl.when(middle & (t >= 8))
        def _():
            z_middle(chunk(t))

        each(s - LH, lambda u, count: activation(chunk1(u), count))
        return carry

    lax.fori_loop(0, LOOPED, step, 0)

    def tail(kind, u):
        n, count = chunk(jnp.int32(u)), 2 if u < 16 else 1
        if kind == "M":
            layer1_last(n, 2 + (u - 16) // 2)
        elif kind == "H":
            activation(n, count)
        elif kind == "F":
            pass_y(n, count)
        elif kind == "C":
            pass_x(n, count)
        elif kind == "L":
            layer2(n, None if u < 16 else True)
        elif kind == "Z":
            pl.when(edge)(lambda: z_edge(n))
            pl.when(middle)(lambda: z_middle(n))
        elif kind == "B":
            pl.when(middle)(lambda: z_back(8 * plane(0) + 2 * u))
        elif kind == "O":
            finish(u)

    for kind, u in TAIL:
        tail(kind, u)

    arrived(o_ref, orr)
    sent(ob.at[pl.ds(0, 6)], oss)
    sent(cs, css)
    for sem, width in ((hys, half), (hxs, 2 * half), (hcs, 4 * half)):
        sent(hb.at[:, :, pl.ds(0, width)], sem)
    sent(zp.at[pl.ds(0, 24)], zss)
    for sem in (xxs, xc0s, xc1s):
        sent(xb.at[pl.ds(0, 4), 0, 0], sem)
    sent(xb.at[pl.ds(0, 12), :, 0], xc2s)

    @pl.when(edge)
    def _():
        sent(xb.at[pl.ds(0, 4), :, 0], xfs)

    @pl.when(middle)
    def _():
        sent(xb.at[pl.ds(0, 8), :, 0], xfs)
        sent(xb.at[pl.ds(0, 12), :, 0], xbs)


def solution(mesh):
    def body(x, w1, w2):
        r, d = x.shape
        k1, n1 = w1.shape
        k2, n2 = w2.shape
        half = n1 // 2
        f32, bf16 = jnp.float32, jnp.bfloat16
        dma = pltpu.SemaphoreType.DMA
        one, four, groups, chunks = dma(()), dma((4,)), dma((16,)), dma((CHUNKS,))
        out = pl.pallas_call(
            kernel,
            out_shape=jax.ShapeDtypeStruct((4, r // 4, d), bf16),
            in_specs=[pl.BlockSpec(memory_space=pltpu.HBM)] * 3,
            out_specs=pl.BlockSpec(memory_space=pl.ANY),
            scratch_shapes=[
                pltpu.VMEM((k1, half), bf16),
                pltpu.VMEM((k1, half), bf16),
                pltpu.VMEM((k2, n2), bf16),
                pltpu.VMEM((16, 2, 2, 16, d), bf16),
                pltpu.VMEM((CHUNKS, ROWS, half), f32),
                pltpu.VMEM((CHUNKS, ROWS, half), f32),
                pltpu.VMEM((CHUNKS, ROWS, half), f32),
                pltpu.VMEM((CHUNKS, ROWS, k2), bf16),
                pltpu.VMEM((CHUNKS, ROWS, n2), f32),
                pltpu.VMEM((CHUNKS, ROWS, n2), f32),
                pltpu.VMEM((CHUNKS, ROWS, n2), f32),
                pltpu.VMEM((8, 2, 16, n2), bf16),
                dma((7,)),
                one, four,
                one, one, groups,
                one, four, one, four, one, groups,
                one, chunks,
                one, chunks,
                one, chunks,
                one, chunks,
                one, chunks, chunks,
                one, one,
            ],
            compiler_params=pltpu.CompilerParams(
                collective_id=0, has_side_effects=True, vmem_limit_bytes=48 * 1024 * 1024),
            name="mlp",
        )(pltpu.with_memory_space_constraint(x, pltpu.HBM), w1, w2)
        return out.reshape(r, d)

    return jax.shard_map(
        body,
        mesh=mesh,
        in_specs=(P(("cx", "cz"), "cy"), P("cy", ("cz", "cx")), P("cz", ("cy", "cx"))),
        out_specs=P(("cx", "cz"), "cy"),
        check_vma=False,
    )
```

```python
import jax
import jax.numpy as jnp
from jax import lax
from jax.experimental import pallas as pl
from jax.experimental.pallas import tpu as pltpu
from jax.sharding import PartitionSpec as P

MESH = pl.DeviceIdType.MESH
CHUNKS, ROWS = 32, 32
LOOPED = 16
LH, LF, LC, L2 = 1, 3, 5, 6
TAIL = (
    ("L", 10), ("F", 13), ("Z", 10), ("C", 11), ("M", 16), ("L", 11), ("H", 15), ("C", 12), ("Z", 11), ("C", 13),
    ("M", 18), ("F", 14), ("L", 12), ("H", 16), ("B", 0), ("Z", 12), ("L", 13), ("H", 17), ("C", 14), ("B", 1),
    ("F", 15), ("Z", 13), ("L", 14), ("H", 18), ("Z", 14), ("B", 2), ("H", 19), ("F", 16), ("C", 15), ("F", 17),
    ("F", 18), ("L", 15), ("Z", 15), ("B", 3), ("F", 19), ("O", 0), ("C", 16), ("C", 17), ("O", 1), ("C", 18),
    ("L", 16), ("C", 19), ("O", 2), ("L", 18), ("O", 3),
)
EDGE = (0, 2, 4, 6, 7, 5, 3, 1)
MIDDLE = (2, 0, 1, 4, 6, 7, 5, 3)
X_EDGE = tuple((3 + e, k, j) for e, (k, j) in enumerate(
    ((1, 0), (1, 1), (2, 0), (2, 1), (3, 0), (3, 1), (3, 2), (3, 3), (2, 2), (2, 3), (1, 2), (1, 3))))
X_BACK = tuple((3 + j, 0, j) for j in range(4))
X_FRONT = tuple((3 + e, k, j) for e, (k, j) in enumerate(
    ((2, 0), (2, 1), (3, 0), (3, 1), (3, 2), (3, 3), (2, 2), (2, 3))))
X_LATE_FRONT = ((7, 2), (8, 3))
X_LATE_BACK = ((10, 2), (11, 3))


def pick(index, pairs, default=0):
    value = jnp.int32(default)
    for key, item in pairs:
        value = jnp.where(index == key, jnp.int32(item), value)
    return value


def kernel(x_ref, w1_ref, w2_ref, o_ref, w1s, w1o, w2, xb, cs, co, cr, hb, zp, zf, zb, ob,
           wsem, xxs, xxr, xfs, xbs, xzr, xc0s, xc0r, xc1s, xc1r, xc2s, xc2r, css, crr, hys, hyr, hxs, hxr,
           hcs, hcr, zss, zfr, zbr, oss, orr):
    p, y, a = lax.axis_index("cz"), lax.axis_index("cy"), lax.axis_index("cx")
    core, ax = lax.rem(a, 2), a // 2
    half = w1s.shape[1]
    a_c, a_x = a + 1 - 2 * core, lax.rem(a + 2, 4)
    a_d = lax.rem(a_c + 2, 4)
    low = p < 2
    edge = (p == 0) | (p == 3)
    middle = (p > 0) & (p < 3)
    ypeer, cpeer, xpeer, dpeer = {"cy": 1 - y}, {"cx": a_c}, {"cx": a_x}, {"cx": a_d}
    front = {"cz": jnp.where(low, p + 1, p - 1)}
    back = {"cz": jnp.where(edge, p, jnp.where(low, p - 1, p + 1))}

    def rcopy(src, dst, ss, rs, device):
        return pltpu.make_async_remote_copy(
            src_ref=src, dst_ref=dst, send_sem=ss, recv_sem=rs, device_id=device, device_id_type=MESH)

    def arrived(ref, sem):
        rcopy(ref, ref, oss, sem, cpeer).wait_recv()

    def sent(ref, sem):
        rcopy(ref, ref, sem, orr, cpeer).wait_send()

    def lanes(owner, width):
        return pl.ds(pl.multiple_of(owner * half, 128), width)

    def plane(k):
        return jnp.where(low, k, 3 - k)

    loads = [
        pltpu.make_async_copy(x_ref.at[pl.ds(16 * j, 16)], xb.at[4 * p + j, ax, core], wsem.at[j]) for j in range(4)]
    loads += [
        pltpu.make_async_copy(w1_ref.at[:, lanes(1 - y, half)], w1s, wsem.at[4]),
        pltpu.make_async_copy(w1_ref.at[:, lanes(y, half)], w1o, wsem.at[5]),
        pltpu.make_async_copy(w2_ref, w2, wsem.at[6]),
    ]
    for load in loads[:5]:
        load.start()

    barrier = pltpu.get_barrier_semaphore()
    for device in (ypeer, cpeer, xpeer, dpeer, front):
        pl.semaphore_signal(barrier, inc=1, device_id=device, device_id_type=MESH)

    @pl.when(middle)
    def _():
        pl.semaphore_signal(barrier, inc=1, device_id=back, device_id_type=MESH)
        pl.semaphore_wait(barrier, 6)

    @pl.when(edge)
    def _():
        pl.semaphore_wait(barrier, 5)

    def x_front(g):
        pair = xb.at[g, :, core]
        rcopy(pair, pair, xfs, xzr.at[g], front).start()

    def x_back(g):
        pair = xb.at[g, :, core]
        rcopy(pair, pair, xbs, xzr.at[g], back).start()

    def x_part(j, owner):
        part = xb.at[4 * p + j, owner, core]
        rcopy(part, part, xfs, xzr.at[4 * p + j], front).start()

        @pl.when(middle)
        def _():
            rcopy(part, part, xbs, xzr.at[4 * p + j], back).start()

    def pair_to_core(g):
        pair = xb.at[g, :, core]
        rcopy(pair, pair, xc2s, xc2r.at[g], cpeer).start()

    def own_arrived(j):
        piece = xb.at[4 * p + j, 1 - ax, core]
        arrived(piece, xxr.at[j])
        rcopy(piece, piece, xc1s, xc1r.at[j], cpeer).start()

        @pl.when(j < 2)
        def _():
            x_part(j, 1 - ax)

        @pl.when(edge & (j >= 2))
        def _():
            x_front(4 * p + j)

    for j in range(4):
        piece = xb.at[4 * p + j, ax, core]
        loads[j].wait()
        rcopy(piece, piece, xc0s, xc0r.at[j], cpeer).start()
        rcopy(piece, piece, xxs, xxr.at[j], xpeer).start()
        if j < 2:
            x_part(j, ax)

    loads[5].start()
    loads[4].wait()

    def chunk(u):
        place = (u - 2) // 2
        base = jnp.where(edge, pick(place, tuple(enumerate(EDGE))), pick(place, tuple(enumerate(MIDDLE))))
        other = 8 * plane(base // 2) + 4 * lax.rem(base, 2) + 2 * lax.rem(u, 2)
        return jnp.where(u < 4, 8 * p + u, jnp.where(u < 16, other, 8 * p + u - 12))

    def chunk1(u):
        turn = u // 2
        first = 8 * p + 2 * lax.rem(u, 2) + turn + ax - 2 * turn * ax
        return jnp.where(u < 4, first, chunk(u))

    def rows_of(ref, n, count):
        return ref.at[pl.ds(n, count)]

    def product(xv, w, count):
        z = jnp.dot(xv.reshape(count * ROWS, xv.shape[-1]), w[...], preferred_element_type=jnp.float32)
        return z.reshape(count, ROWS, z.shape[1])

    def layer1(n, count, start):
        g, h = n // 2, lax.rem(n, 2)
        if count == 2:
            arrived(xb.at[g, :, 1 - core], xc2r.at[g])
            xv = xb[g]
            cs[pl.ds(n, count)] = product(xv, w1s, count)
            rcopy(rows_of(cs, n, count), rows_of(cr, n, count), css, crr.at[n], ypeer).start()
        else:
            j = lax.rem(g, 4)

            def part(c):
                rows = pl.ds(pl.multiple_of(16 * c, 16), 16)
                cs[n, rows] = jnp.dot(xb[g, h, c], w1s[...], preferred_element_type=jnp.float32)
                rcopy(cs.at[n, rows], cr.at[n, rows], css, crr.at[n], ypeer).start()

            part(core)

            @pl.when(h == ax)
            def _():
                arrived(xb.at[g, h, 1 - core], xc0r.at[j])

            @pl.when(h != ax)
            def _():
                arrived(xb.at[g, h, 1 - core], xc1r.at[j])

            part(1 - core)
            xv = xb[g, h]

            @pl.when(start)
            def _():
                loads[5].wait()
                loads[6].start()

        co[pl.ds(n, count)] = product(xv, w1o, count)

    def layer1_last(n, j):
        arrived(xb.at[4 * p + j, ax, 1 - core], xc0r.at[j])
        arrived(xb.at[4 * p + j, 1 - ax, 1 - core], xc1r.at[j])
        xv = xb[4 * p + j]
        cs[pl.ds(n, 2)] = product(xv, w1s, 2)
        for i in range(2):
            rcopy(rows_of(cs, n + i, 1), rows_of(cr, n + i, 1), css, crr.at[n + i], ypeer).start()
        co[pl.ds(n, 2)] = product(xv, w1o, 2)

    def h_piece(n, count, owner, width):
        return hb.at[pl.ds(n, count), :, lanes(owner, width)]

    def activation(n, count):
        arrived(rows_of(cr, n, count), crr.at[n])
        c = (co[pl.ds(n, count)] + cr[pl.ds(n, count)]).astype(jnp.bfloat16).astype(jnp.float32)
        h = jax.nn.gelu(c, approximate=True).astype(jnp.bfloat16)
        hb[pl.ds(n, count), :, lanes(2 * a + y, half)] = h
        piece = h_piece(n, count, 2 * a + y, half)
        rcopy(piece, piece, hys, hyr.at[n], ypeer).start()
        rcopy(piece, piece, hxs, hxr.at[n], xpeer).start()

    def pass_y(n, count):
        piece = h_piece(n, count, 2 * a + 1 - y, half)
        arrived(piece, hyr.at[n])
        rcopy(piece, piece, hxs, hxr.at[n], xpeer).start()
        piece = h_piece(n, count, 2 * a, 2 * half)
        rcopy(piece, piece, hcs, hcr.at[n], cpeer).start()

    def pass_x(n, count):
        piece = h_piece(n, count, 2 * a_x, 2 * half)
        arrived(piece, hxr.at[n])
        rcopy(piece, piece, hcs, hcr.at[n], cpeer).start()

    def layer2(n, own):
        if own is None:
            arrived(h_piece(n, 2, 0, 4 * half), hcr.at[n])
        elif own is True:
            arrived(h_piece(n, 1, 0, 4 * half), hcr.at[n])
            arrived(h_piece(n + 1, 1, 0, 4 * half), hcr.at[n + 1])
        else:
            @pl.when(own)
            def _():
                arrived(h_piece(n, 1, 0, 4 * half), hcr.at[n])
                arrived(h_piece(n + 1, 1, 0, 4 * half), hcr.at[n + 1])

            @pl.when(jnp.logical_not(own))
            def _():
                arrived(h_piece(n, 2, 0, 4 * half), hcr.at[n])

        zp[pl.ds(n, 2)] = product(hb[pl.ds(n, 2)], w2, 2)

    def z_send(n, to, sems, device):
        rcopy(rows_of(zp, n, 2), rows_of(to, n, 2), zss, sems.at[n], device).start()

    def add(n, count, ref):
        zp[pl.ds(n, count)] = zp[pl.ds(n, count)] + ref[pl.ds(n, count)]

    def out_piece(i, c, j, device):
        rcopy(ob.at[i, c], o_ref.at[j, :, lanes(a, half)], oss, orr, device).start()

    def out_own(i, j):
        pltpu.make_async_copy(ob.at[i, core], o_ref.at[j, :, lanes(a, half)], orr).start()
        out_piece(i, 1 - core, j, cpeer)

    def out_other(i, j):
        out_piece(i, core, j, xpeer)
        out_piece(i, 1 - core, j, dpeer)

    def partials_arrived(n):
        arrived(rows_of(zf, n, 2), zfr.at[n])

        @pl.when(middle)
        def _():
            arrived(rows_of(zb, n, 2), zbr.at[n])

    def finish(j):
        n = 8 * p + 2 * j
        partials_arrived(n)
        add(n, 2, zf)

        @pl.when(middle)
        def _():
            add(n, 2, zb)

        ob[pl.ds(2 * j, 2)] = zp[pl.ds(n, 2)].astype(jnp.bfloat16).reshape((2,) + ob.shape[1:])
        out_other(2 * j + 1 - ax, j)
        out_own(2 * j + ax, j)

    def z_edge(n):
        z_send(n, zb, zbr, front)

    def z_middle(n):
        arrived(rows_of(zb, n, 2), zbr.at[n])
        add(n, 2, zb)
        z_send(n, zf, zfr, front)

    def z_back(n):
        arrived(rows_of(zf, n, 2), zfr.at[n])
        add(n, 2, zf)
        z_send(n, zf, zfr, back)

    def step(s, carry):
        def each(u, event):
            @pl.when((u >= 0) & (u < 4))
            def _():
                event(u, 1)

            @pl.when(u >= 4)
            def _():
                event(u, 2)

        each(s, lambda u, count: layer1(chunk1(u), count, s == 0))
        each(s - LF, lambda u, count: pass_y(chunk1(u), count))

        @pl.when((s >= 1) & (s < 5))
        def _():
            own_arrived(s - 1)

        group = pick(s, [(at, 4 * k + j) for at, k, j in X_EDGE], -1)

        @pl.when(edge & (group >= 0))
        def _():
            g = 4 * plane(group // 4) + lax.rem(group, 4)
            arrived(xb.at[g, :, core], xzr.at[g])
            pair_to_core(g)

        group_b = pick(s, [(at, 4 * k + j) for at, k, j in X_BACK], -1)

        @pl.when(middle & (group_b >= 0))
        def _():
            g = 4 * plane(group_b // 4) + lax.rem(group_b, 4)
            arrived(xb.at[g, :, core], xzr.at[g])
            x_front(g)
            pair_to_core(g)

        group_f = pick(s, [(at, 4 * k + j) for at, k, j in X_FRONT], -1)

        @pl.when(middle & (group_f >= 0))
        def _():
            g = 4 * plane(group_f // 4) + lax.rem(group_f, 4)
            arrived(xb.at[g, :, core], xzr.at[g])
            x_back(g)
            pair_to_core(g)

        for order, send in ((X_LATE_FRONT, x_front), (X_LATE_BACK, x_back)):
            late = pick(s, order, -1)

            @pl.when(middle & (late >= 0))
            def _():
                send(4 * p + late)

        each(s - LC, lambda u, count: pass_x(chunk(u), count))

        t = s - L2

        @pl.when(t == 1)
        def _():
            loads[6].wait()

        @pl.when((t == 1) | (t >= 3))
        def _():
            layer2(chunk(jnp.where(t < 4, t - 1, t)), t < 4)

        @pl.when(edge & (t >= 4))
        def _():
            z_edge(chunk(t))

        @pl.when(middle & (t >= 8))
        def _():
            z_middle(chunk(t))

        each(s - LH, lambda u, count: activation(chunk1(u), count))
        return carry

    lax.fori_loop(0, LOOPED, step, 0)

    def tail(kind, u):
        n, count = chunk(jnp.int32(u)), 2 if u < 16 else 1
        if kind == "M":
            layer1_last(n, 2 + (u - 16) // 2)
        elif kind == "H":
            activation(n, count)
        elif kind == "F":
            pass_y(n, count)
        elif kind == "C":
            pass_x(n, count)
        elif kind == "L":
            layer2(n, None if u < 16 else True)
        elif kind == "Z":
            pl.when(edge)(lambda: z_edge(n))
            pl.when(middle)(lambda: z_middle(n))
        elif kind == "B":
            pl.when(middle)(lambda: z_back(8 * plane(0) + 2 * u))
        elif kind == "O":
            finish(u)

    for kind, u in TAIL:
        tail(kind, u)

    sent(cs, css)
    for sem, width in ((hys, half), (hxs, 2 * half), (hcs, 4 * half)):
        sent(hb.at[:, :, pl.ds(0, width)], sem)
    sent(zp.at[pl.ds(0, 24)], zss)
    for sem in (xxs, xc0s, xc1s):
        sent(xb.at[pl.ds(0, 4), 0, 0], sem)
    sent(xb.at[pl.ds(0, 12), :, 0], xc2s)

    @pl.when(edge)
    def _():
        sent(xb.at[pl.ds(0, 4), :, 0], xfs)

    @pl.when(middle)
    def _():
        sent(xb.at[pl.ds(0, 8), :, 0], xfs)
        sent(xb.at[pl.ds(0, 12), :, 0], xbs)

    sent(ob.at[pl.ds(0, 6)], oss)
    arrived(o_ref, orr)


def solution(mesh):
    def body(x, w1, w2):
        r, d = x.shape
        k1, n1 = w1.shape
        k2, n2 = w2.shape
        half = n1 // 2
        f32, bf16 = jnp.float32, jnp.bfloat16
        dma = pltpu.SemaphoreType.DMA
        one, four, groups, chunks = dma(()), dma((4,)), dma((16,)), dma((CHUNKS,))
        out = pl.pallas_call(
            kernel,
            out_shape=jax.ShapeDtypeStruct((4, r // 4, d), bf16),
            in_specs=[pl.BlockSpec(memory_space=pltpu.HBM)] * 3,
            out_specs=pl.BlockSpec(memory_space=pl.ANY),
            scratch_shapes=[
                pltpu.VMEM((k1, half), bf16),
                pltpu.VMEM((k1, half), bf16),
                pltpu.VMEM((k2, n2), bf16),
                pltpu.VMEM((16, 2, 2, 16, d), bf16),
                pltpu.VMEM((CHUNKS, ROWS, half), f32),
                pltpu.VMEM((CHUNKS, ROWS, half), f32),
                pltpu.VMEM((CHUNKS, ROWS, half), f32),
                pltpu.VMEM((CHUNKS, ROWS, k2), bf16),
                pltpu.VMEM((CHUNKS, ROWS, n2), f32),
                pltpu.VMEM((CHUNKS, ROWS, n2), f32),
                pltpu.VMEM((CHUNKS, ROWS, n2), f32),
                pltpu.VMEM((8, 2, 16, n2), bf16),
                dma((7,)),
                one, four,
                one, one, groups,
                one, four, one, four, one, groups,
                one, chunks,
                one, chunks,
                one, chunks,
                one, chunks,
                one, chunks, chunks,
                one, one,
            ],
            compiler_params=pltpu.CompilerParams(
                collective_id=0, has_side_effects=True, vmem_limit_bytes=48 * 1024 * 1024),
            name="mlp",
        )(pltpu.with_memory_space_constraint(x, pltpu.HBM), w1, w2)
        return out.reshape(r, d)

    return jax.shard_map(
        body,
        mesh=mesh,
        in_specs=(P(("cx", "cz"), "cy"), P("cy", ("cz", "cx")), P("cz", ("cy", "cx"))),
        out_specs=P(("cx", "cz"), "cy"),
        check_vma=False,
    )
```

```python
import jax
import jax.numpy as jnp
from jax import lax
from jax.experimental import pallas as pl
from jax.experimental.pallas import tpu as pltpu
from jax.sharding import PartitionSpec as P

MESH = pl.DeviceIdType.MESH
CHUNKS, ROWS = 32, 32
LOOPED = 16
LH, LF, LC, L2 = 1, 3, 5, 6
TAIL = (
    ("L", 10), ("F", 13), ("Z", 10), ("C", 11), ("M", 16), ("L", 11), ("H", 15), ("C", 12), ("Z", 11), ("C", 13),
    ("M", 18), ("F", 14), ("L", 12), ("H", 16), ("B", 0), ("Z", 12), ("L", 13), ("H", 17), ("C", 14), ("B", 1),
    ("F", 15), ("Z", 13), ("L", 14), ("H", 18), ("Z", 14), ("B", 2), ("H", 19), ("F", 16), ("C", 15), ("F", 17),
    ("F", 18), ("L", 15), ("Z", 15), ("B", 3), ("F", 19), ("O", 0), ("C", 16), ("C", 17), ("O", 1), ("C", 18),
    ("L", 16), ("C", 19), ("O", 2), ("L", 18), ("O", 3),
)
EDGE = (0, 2, 4, 6, 7, 5, 3, 1)
MIDDLE = (2, 0, 1, 4, 6, 7, 5, 3)
X_EDGE = tuple((3 + e, k, j) for e, (k, j) in enumerate(
    ((1, 0), (1, 1), (2, 0), (2, 1), (3, 0), (3, 1), (3, 2), (3, 3), (2, 2), (2, 3), (1, 2), (1, 3))))
X_BACK = tuple((3 + j, 0, j) for j in range(4))
X_FRONT = tuple((3 + e, k, j) for e, (k, j) in enumerate(
    ((2, 0), (2, 1), (3, 0), (3, 1), (3, 2), (3, 3), (2, 2), (2, 3))))
X_LATE_FRONT = ((7, 2), (8, 3))
X_LATE_BACK = ((10, 2), (11, 3))


def pick(index, pairs, default=0):
    value = jnp.int32(default)
    for key, item in pairs:
        value = jnp.where(index == key, jnp.int32(item), value)
    return value


def kernel(x_ref, w1_ref, w2_ref, o_ref, w1s, w1o, w2, xb, cs, co, cr, hb, zp, zf, zb, ob,
           wsem, xxs, xxr, xfs, xbs, xzr, xc0s, xc0r, xc1s, xc1r, xc2s, xc2r, css, crr, hys, hyr, hxs, hxr,
           hcs, hcr, zss, zfr, zbr, oss, orr):
    p, y, a = lax.axis_index("cz"), lax.axis_index("cy"), lax.axis_index("cx")
    core, ax = lax.rem(a, 2), a // 2
    half = w1s.shape[1]
    a_c, a_x = a + 1 - 2 * core, lax.rem(a + 2, 4)
    a_d = lax.rem(a_c + 2, 4)
    low = p < 2
    edge = (p == 0) | (p == 3)
    middle = (p > 0) & (p < 3)
    ypeer, cpeer, xpeer, dpeer = {"cy": 1 - y}, {"cx": a_c}, {"cx": a_x}, {"cx": a_d}
    front = {"cz": jnp.where(low, p + 1, p - 1)}
    back = {"cz": jnp.where(edge, p, jnp.where(low, p - 1, p + 1))}

    def rcopy(src, dst, ss, rs, device):
        return pltpu.make_async_remote_copy(
            src_ref=src, dst_ref=dst, send_sem=ss, recv_sem=rs, device_id=device, device_id_type=MESH)

    def arrived(ref, sem):
        rcopy(ref, ref, oss, sem, cpeer).wait_recv()

    def sent(ref, sem):
        rcopy(ref, ref, sem, orr, cpeer).wait_send()

    def lanes(owner, width):
        return pl.ds(pl.multiple_of(owner * half, 128), width)

    def plane(k):
        return jnp.where(low, k, 3 - k)

    loads = [
        pltpu.make_async_copy(x_ref.at[pl.ds(16 * j, 16)], xb.at[4 * p + j, ax, core], wsem.at[j]) for j in range(4)]
    loads += [
        pltpu.make_async_copy(w1_ref.at[:, lanes(1 - y, half)], w1s, wsem.at[4]),
        pltpu.make_async_copy(w1_ref.at[:, lanes(y, half)], w1o, wsem.at[5]),
        pltpu.make_async_copy(w2_ref, w2, wsem.at[6]),
    ]
    for load in loads[:6]:
        load.start()

    barrier = pltpu.get_barrier_semaphore()
    for device in (ypeer, cpeer, xpeer, dpeer, front):
        pl.semaphore_signal(barrier, inc=1, device_id=device, device_id_type=MESH)

    @pl.when(middle)
    def _():
        pl.semaphore_signal(barrier, inc=1, device_id=back, device_id_type=MESH)
        pl.semaphore_wait(barrier, 6)

    @pl.when(edge)
    def _():
        pl.semaphore_wait(barrier, 5)

    def x_front(g):
        pair = xb.at[g, :, core]
        rcopy(pair, pair, xfs, xzr.at[g], front).start()

    def x_back(g):
        pair = xb.at[g, :, core]
        rcopy(pair, pair, xbs, xzr.at[g], back).start()

    def x_part(j, owner):
        part = xb.at[4 * p + j, owner, core]
        rcopy(part, part, xfs, xzr.at[4 * p + j], front).start()

        @pl.when(middle)
        def _():
            rcopy(part, part, xbs, xzr.at[4 * p + j], back).start()

    def pair_to_core(g):
        pair = xb.at[g, :, core]
        rcopy(pair, pair, xc2s, xc2r.at[g], cpeer).start()

    def own_arrived(j):
        piece = xb.at[4 * p + j, 1 - ax, core]
        arrived(piece, xxr.at[j])
        rcopy(piece, piece, xc1s, xc1r.at[j], cpeer).start()

        @pl.when(j < 2)
        def _():
            x_part(j, 1 - ax)

        @pl.when(edge & (j >= 2))
        def _():
            x_front(4 * p + j)

    for j in range(4):
        piece = xb.at[4 * p + j, ax, core]
        loads[j].wait()
        rcopy(piece, piece, xc0s, xc0r.at[j], cpeer).start()
        rcopy(piece, piece, xxs, xxr.at[j], xpeer).start()
        if j < 2:
            x_part(j, ax)

    loads[4].wait()
    loads[6].start()

    def chunk(u):
        place = (u - 2) // 2
        base = jnp.where(edge, pick(place, tuple(enumerate(EDGE))), pick(place, tuple(enumerate(MIDDLE))))
        other = 8 * plane(base // 2) + 4 * lax.rem(base, 2) + 2 * lax.rem(u, 2)
        return jnp.where(u < 4, 8 * p + u, jnp.where(u < 16, other, 8 * p + u - 12))

    def chunk1(u):
        turn = u // 2
        first = 8 * p + 2 * lax.rem(u, 2) + turn + ax - 2 * turn * ax
        return jnp.where(u < 4, first, chunk(u))

    def rows_of(ref, n, count):
        return ref.at[pl.ds(n, count)]

    def product(xv, w, count):
        z = jnp.dot(xv.reshape(count * ROWS, xv.shape[-1]), w[...], preferred_element_type=jnp.float32)
        return z.reshape(count, ROWS, z.shape[1])

    def layer1(n, count, start, split):
        g, h = n // 2, lax.rem(n, 2)
        if count == 2:
            arrived(xb.at[g, :, 1 - core], xc2r.at[g])
            xv = xb[g]
            cs[pl.ds(n, count)] = product(xv, w1s, count)
            rcopy(rows_of(cs, n, count), rows_of(cr, n, count), css, crr.at[n], ypeer).start()
        else:
            j = lax.rem(g, 4)

            def part(c):
                rows = pl.ds(pl.multiple_of(16 * c, 16), 16)
                cs[n, rows] = jnp.dot(xb[g, h, c], w1s[...], preferred_element_type=jnp.float32)
                rcopy(cs.at[n, rows], cr.at[n, rows], css, crr.at[n], ypeer).start()

            pl.when(split)(lambda: part(core))

            @pl.when(h == ax)
            def _():
                arrived(xb.at[g, h, 1 - core], xc0r.at[j])

            @pl.when(h != ax)
            def _():
                arrived(xb.at[g, h, 1 - core], xc1r.at[j])

            pl.when(split)(lambda: part(1 - core))

            @pl.when(jnp.logical_not(split))
            def _():
                cs[pl.ds(n, 1)] = product(xb[g, h], w1s, 1)
                rcopy(rows_of(cs, n, 1), rows_of(cr, n, 1), css, crr.at[n], ypeer).start()

            xv = xb[g, h]

            @pl.when(start)
            def _():
                loads[5].wait()

        co[pl.ds(n, count)] = product(xv, w1o, count)

    def layer1_last(n, j):
        arrived(xb.at[4 * p + j, ax, 1 - core], xc0r.at[j])
        arrived(xb.at[4 * p + j, 1 - ax, 1 - core], xc1r.at[j])
        xv = xb[4 * p + j]
        cs[pl.ds(n, 2)] = product(xv, w1s, 2)
        for i in range(2):
            rcopy(rows_of(cs, n + i, 1), rows_of(cr, n + i, 1), css, crr.at[n + i], ypeer).start()
        co[pl.ds(n, 2)] = product(xv, w1o, 2)

    def h_piece(n, count, owner, width):
        return hb.at[pl.ds(n, count), :, lanes(owner, width)]

    def activation(n, count):
        arrived(rows_of(cr, n, count), crr.at[n])
        c = (co[pl.ds(n, count)] + cr[pl.ds(n, count)]).astype(jnp.bfloat16).astype(jnp.float32)
        h = jax.nn.gelu(c, approximate=True).astype(jnp.bfloat16)
        hb[pl.ds(n, count), :, lanes(2 * a + y, half)] = h
        piece = h_piece(n, count, 2 * a + y, half)
        rcopy(piece, piece, hys, hyr.at[n], ypeer).start()
        rcopy(piece, piece, hxs, hxr.at[n], xpeer).start()

    def pass_y(n, count):
        piece = h_piece(n, count, 2 * a + 1 - y, half)
        arrived(piece, hyr.at[n])
        rcopy(piece, piece, hxs, hxr.at[n], xpeer).start()
        piece = h_piece(n, count, 2 * a, 2 * half)
        rcopy(piece, piece, hcs, hcr.at[n], cpeer).start()

    def pass_x(n, count):
        piece = h_piece(n, count, 2 * a_x, 2 * half)
        arrived(piece, hxr.at[n])
        rcopy(piece, piece, hcs, hcr.at[n], cpeer).start()

    def layer2(n, own):
        if own is None:
            arrived(h_piece(n, 2, 0, 4 * half), hcr.at[n])
        elif own is True:
            arrived(h_piece(n, 1, 0, 4 * half), hcr.at[n])
            arrived(h_piece(n + 1, 1, 0, 4 * half), hcr.at[n + 1])
        else:
            @pl.when(own)
            def _():
                arrived(h_piece(n, 1, 0, 4 * half), hcr.at[n])
                arrived(h_piece(n + 1, 1, 0, 4 * half), hcr.at[n + 1])

            @pl.when(jnp.logical_not(own))
            def _():
                arrived(h_piece(n, 2, 0, 4 * half), hcr.at[n])

        zp[pl.ds(n, 2)] = product(hb[pl.ds(n, 2)], w2, 2)

    def z_send(n, to, sems, device):
        rcopy(rows_of(zp, n, 2), rows_of(to, n, 2), zss, sems.at[n], device).start()

    def add(n, count, ref):
        zp[pl.ds(n, count)] = zp[pl.ds(n, count)] + ref[pl.ds(n, count)]

    def out_piece(i, c, j, device):
        rcopy(ob.at[i, c], o_ref.at[j, :, lanes(a, half)], oss, orr, device).start()

    def out_own(i, j):
        pltpu.make_async_copy(ob.at[i, core], o_ref.at[j, :, lanes(a, half)], orr).start()
        out_piece(i, 1 - core, j, cpeer)

    def out_other(i, j):
        out_piece(i, core, j, xpeer)
        out_piece(i, 1 - core, j, dpeer)

    def partials_arrived(n):
        arrived(rows_of(zf, n, 2), zfr.at[n])

        @pl.when(middle)
        def _():
            arrived(rows_of(zb, n, 2), zbr.at[n])

    def finish(j):
        n = 8 * p + 2 * j
        partials_arrived(n)
        add(n, 2, zf)

        @pl.when(middle)
        def _():
            add(n, 2, zb)

        ob[pl.ds(2 * j, 2)] = zp[pl.ds(n, 2)].astype(jnp.bfloat16).reshape((2,) + ob.shape[1:])
        out_other(2 * j + 1 - ax, j)
        out_own(2 * j + ax, j)

    def z_edge(n):
        z_send(n, zb, zbr, front)

    def z_middle(n):
        arrived(rows_of(zb, n, 2), zbr.at[n])
        add(n, 2, zb)
        z_send(n, zf, zfr, front)

    def z_back(n):
        arrived(rows_of(zf, n, 2), zfr.at[n])
        add(n, 2, zf)
        z_send(n, zf, zfr, back)

    def step(s, carry):
        def each(u, event):
            @pl.when((u >= 0) & (u < 4))
            def _():
                event(u, 1)

            @pl.when(u >= 4)
            def _():
                event(u, 2)

        each(s, lambda u, count: layer1(chunk1(u), count, s == 0, lax.rem(s, 2) == 0))
        each(s - LF, lambda u, count: pass_y(chunk1(u), count))

        @pl.when((s >= 1) & (s < 5))
        def _():
            own_arrived(s - 1)

        group = pick(s, [(at, 4 * k + j) for at, k, j in X_EDGE], -1)

        @pl.when(edge & (group >= 0))
        def _():
            g = 4 * plane(group // 4) + lax.rem(group, 4)
            arrived(xb.at[g, :, core], xzr.at[g])
            pair_to_core(g)

        group_b = pick(s, [(at, 4 * k + j) for at, k, j in X_BACK], -1)

        @pl.when(middle & (group_b >= 0))
        def _():
            g = 4 * plane(group_b // 4) + lax.rem(group_b, 4)
            arrived(xb.at[g, :, core], xzr.at[g])
            x_front(g)
            pair_to_core(g)

        group_f = pick(s, [(at, 4 * k + j) for at, k, j in X_FRONT], -1)

        @pl.when(middle & (group_f >= 0))
        def _():
            g = 4 * plane(group_f // 4) + lax.rem(group_f, 4)
            arrived(xb.at[g, :, core], xzr.at[g])
            x_back(g)
            pair_to_core(g)

        for order, send in ((X_LATE_FRONT, x_front), (X_LATE_BACK, x_back)):
            late = pick(s, order, -1)

            @pl.when(middle & (late >= 0))
            def _():
                send(4 * p + late)

        each(s - LC, lambda u, count: pass_x(chunk(u), count))

        t = s - L2

        @pl.when(t == 1)
        def _():
            loads[6].wait()

        @pl.when((t == 1) | (t >= 3))
        def _():
            layer2(chunk(jnp.where(t < 4, t - 1, t)), t < 4)

        @pl.when(edge & (t >= 4))
        def _():
            z_edge(chunk(t))

        @pl.when(middle & (t >= 8))
        def _():
            z_middle(chunk(t))

        each(s - LH, lambda u, count: activation(chunk1(u), count))
        return carry

    lax.fori_loop(0, LOOPED, step, 0)

    def tail(kind, u):
        n, count = chunk(jnp.int32(u)), 2 if u < 16 else 1
        if kind == "M":
            layer1_last(n, 2 + (u - 16) // 2)
        elif kind == "H":
            activation(n, count)
        elif kind == "F":
            pass_y(n, count)
        elif kind == "C":
            pass_x(n, count)
        elif kind == "L":
            layer2(n, None if u < 16 else True)
        elif kind == "Z":
            pl.when(edge)(lambda: z_edge(n))
            pl.when(middle)(lambda: z_middle(n))
        elif kind == "B":
            pl.when(middle)(lambda: z_back(8 * plane(0) + 2 * u))
        elif kind == "O":
            finish(u)

    for kind, u in TAIL:
        tail(kind, u)

    sent(cs, css)
    for sem, width in ((hys, half), (hxs, 2 * half), (hcs, 4 * half)):
        sent(hb.at[:, :, pl.ds(0, width)], sem)
    sent(zp.at[pl.ds(0, 24)], zss)
    for sem in (xxs, xc0s, xc1s):
        sent(xb.at[pl.ds(0, 4), 0, 0], sem)
    sent(xb.at[pl.ds(0, 12), :, 0], xc2s)

    @pl.when(edge)
    def _():
        sent(xb.at[pl.ds(0, 4), :, 0], xfs)

    @pl.when(middle)
    def _():
        sent(xb.at[pl.ds(0, 8), :, 0], xfs)
        sent(xb.at[pl.ds(0, 12), :, 0], xbs)

    sent(ob.at[pl.ds(0, 6)], oss)
    arrived(o_ref, orr)


def solution(mesh):
    def body(x, w1, w2):
        r, d = x.shape
        k1, n1 = w1.shape
        k2, n2 = w2.shape
        half = n1 // 2
        f32, bf16 = jnp.float32, jnp.bfloat16
        dma = pltpu.SemaphoreType.DMA
        one, four, groups, chunks = dma(()), dma((4,)), dma((16,)), dma((CHUNKS,))
        out = pl.pallas_call(
            kernel,
            out_shape=jax.ShapeDtypeStruct((4, r // 4, d), bf16),
            in_specs=[pl.BlockSpec(memory_space=pltpu.HBM)] * 3,
            out_specs=pl.BlockSpec(memory_space=pl.ANY),
            scratch_shapes=[
                pltpu.VMEM((k1, half), bf16),
                pltpu.VMEM((k1, half), bf16),
                pltpu.VMEM((k2, n2), bf16),
                pltpu.VMEM((16, 2, 2, 16, d), bf16),
                pltpu.VMEM((CHUNKS, ROWS, half), f32),
                pltpu.VMEM((CHUNKS, ROWS, half), f32),
                pltpu.VMEM((CHUNKS, ROWS, half), f32),
                pltpu.VMEM((CHUNKS, ROWS, k2), bf16),
                pltpu.VMEM((CHUNKS, ROWS, n2), f32),
                pltpu.VMEM((CHUNKS, ROWS, n2), f32),
                pltpu.VMEM((CHUNKS, ROWS, n2), f32),
                pltpu.VMEM((8, 2, 16, n2), bf16),
                dma((7,)),
                one, four,
                one, one, groups,
                one, four, one, four, one, groups,
                one, chunks,
                one, chunks,
                one, chunks,
                one, chunks,
                one, chunks, chunks,
                one, one,
            ],
            compiler_params=pltpu.CompilerParams(
                collective_id=0, has_side_effects=True, vmem_limit_bytes=48 * 1024 * 1024),
            name="mlp",
        )(pltpu.with_memory_space_constraint(x, pltpu.HBM), w1, w2)
        return out.reshape(r, d)

    return jax.shard_map(
        body,
        mesh=mesh,
        in_specs=(P(("cx", "cz"), "cy"), P("cy", ("cz", "cx")), P("cz", ("cy", "cx"))),
        out_specs=P(("cx", "cz"), "cy"),
        check_vma=False,
    )
```
